32 devices in a mesh: dev: 32 (over z, y, x, core).
Axes of the slice: x: 2, y: 2, z: 4, core: 2. Of those that a mesh axis runs over, the one named last changes fastest.
Arguments:
- pixels: float32 [4, 512, 8192], P(None, 'dev'), may hold values from -10 to 10
- valid_flags: int32 [4, 512, 8192], P(None, 'dev'), may hold values 0 or 1
Outputs:
- tile_halves: float32 [32, 256, 2048], P('dev')
- header: float32 [5, 4], replicated
The draws below stay inside these ranges and needn't reach their ends.
All inputs are finite; a program needn't handle non-finite values. No bound on the sum of `valid_flags` on one device may be relied on, other than what follows from the above.
Results may differ from the reference program's by a relative error of at most 0.00002.
Values sent between devices are 32-bit elements; how exact they have to be, the bound alone decides.
A program may use at most 128 MiB of HBM per device.

```python
import jax
import jax.numpy as jnp
from jax import lax

BANDS = 4
TILE = 512
STRIP = 16
GROUP = 16
COLS = 8192
ROWS = 512
HALF = 256
N_DEV = 32


def draw_pixels(key, part):
    first_key, second_key, third_key = jax.random.split(jax.random.fold_in(key, 11), 3)
    strip_count = ROWS // STRIP
    offsets = jax.random.uniform(first_key, (BANDS, strip_count, 1, 1), jnp.float32, -2.0, 2.0)
    widths = jnp.exp(jax.random.uniform(second_key, (BANDS, strip_count, 1, 1), jnp.float32, jnp.log(0.5), jnp.log(2.0)))
    noise = jnp.clip(jax.random.normal(third_key, (BANDS, strip_count, STRIP, COLS), jnp.float32), -4.0, 4.0)
    values = offsets + widths * noise
    return values.reshape(BANDS, ROWS, COLS).astype(jnp.float32)


def set_ends(result, own_key, low, high):
    longest = result.shape.index(max(result.shape))
    spots = []
    for shift in (0, 1):
        where = [jax.random.randint(jax.random.fold_in(own_key, axis), (), 0, length) for axis, length in enumerate(result.shape)]
        where[longest] = (where[longest] + shift) % result.shape[longest]
        spots.append(tuple(where))
    return result.at[spots[0]].set(low).at[spots[1]].set(high)


def setup_inputs(seed: int = 0) -> dict:
    streams_of = jax.random.split(jax.random.key(seed), 3)
    pixels = draw_pixels(jax.random.fold_in(streams_of[2], 71), 0)
    valid_flags = set_ends((jax.random.randint(streams_of[1], (BANDS, ROWS, COLS), 0, 4) < 3).astype(jnp.int32), jax.random.fold_in(streams_of[1], 1), 0, 1)
    return dict(pixels=pixels, valid_flags=valid_flags)


largest_value = 3e+38

def reference(pixels, valid_flags):
    usable = valid_flags == 1
    filled = jnp.where(usable, pixels, jnp.float32(0.0))
    blocks = filled.reshape(BANDS, ROWS // HALF, HALF, GROUP, TILE)
    tile_halves = jnp.transpose(blocks, (1, 3, 2, 4, 0)).reshape(N_DEV, HALF, TILE * BANDS)
    lowest = lax.optimization_barrier(jnp.min(jnp.where(usable, pixels, jnp.float32(largest_value)), axis=(1, 2)))
    highest = lax.optimization_barrier(jnp.max(jnp.where(usable, pixels, jnp.float32(-largest_value)), axis=(1, 2)))
    valid_count = lax.optimization_barrier(jnp.sum(usable.astype(jnp.float32), axis=(1, 2)))
    band_sum = lax.optimization_barrier(jnp.sum(filled, axis=(1, 2)))
    band_squares = lax.optimization_barrier(jnp.sum(filled * filled, axis=(1, 2)))
    divisor = jnp.maximum(valid_count, 1.0)
    average = band_sum / divisor
    variance = band_squares / divisor - average * average
    header = jnp.stack([lowest, highest, valid_count / (ROWS * COLS), average, jnp.sqrt(jnp.maximum(variance, 0.25))])
    return (tile_halves, header)
```

```python
import functools

import jax
import jax.numpy as jnp
from jax import lax
from jax.experimental import pallas as pl
from jax.experimental.pallas import tpu as pltpu
from jax.sharding import PartitionSpec as P

TILE = 512
LANES = 128
SUBLANES = 8
STATS = 5
SLOT = 8
WINDOW = 3
EARLY = 2

largest_value = 3e38


def partner_of(position, mask, bits):
    partner = position
    for bit in range(bits):
        own = position // (1 << bit) % 2
        flip = mask // (1 << bit) % 2
        partner = partner + flip * (1 - 2 * own) * (1 << bit)
    return partner


def schedule(members):
    whole = members // 2 - 1
    pairs = sorted((min(high, whole - high, key=lambda h: (-h.bit_count(), h))
                    for high in range(1, whole // 2 + 1)))
    groups = [[(whole, 1)], [(whole, 0)]]
    groups += [[(a, core), (whole - a, core)] for a in pairs for core in (0, 1)]
    groups.append([(0, 1)])
    masks, slots = [], []
    for group in groups:
        slots.append(range(len(masks), len(masks) + len(group)))
        masks += [high * 2 + core for high, core in group]
    return masks + [0], slots


def lane_tables(bands):
    block = LANES // bands
    lane = lax.broadcasted_iota(jnp.int32, (SUBLANES, LANES), 1)
    m, r = lane // bands, lane % bands
    spread = [(r - b + bands) % bands * block + m for b in range(bands)]
    fix = [m * bands + (r + j) % bands for j in range(bands)]
    return r, spread, fix


def permute(x, index):
    return jnp.take_along_axis(x, index, axis=1, mode="promise_in_bounds")


def merge_rows(stats):
    which = lax.broadcasted_iota(jnp.int32, (1, LANES), 1) % SLOT
    low = jnp.min(stats, axis=0, keepdims=True)
    high = jnp.max(stats, axis=0, keepdims=True)
    total = jnp.sum(stats, axis=0, keepdims=True)
    return jnp.where(which == 0, low, jnp.where(which == 1, high, total))


def exchange(n, members, early, pix_ref, flag_ref, out_ref, stat_out, pix, flag, send, row, rows_in,
             load_sem, send_sem, recv_sem, row_send, row_recv):
    bands, rows, _ = pix_ref.shape
    bits = members.bit_length() - 1
    me = lax.axis_index("dev")
    position = me % members
    first = me - position

    barrier = pltpu.get_barrier_semaphore()

    groups = n // members

    def mate(k):
        return first + (position + k) % members

    def twin(k):
        return (me + k * members) % n

    def greet(k, whose):
        pl.semaphore_signal(barrier, inc=1, device_id=(whose(k),),
                            device_id_type=pl.DeviceIdType.MESH)

    def greet_mate(k, _):
        greet(k, mate)
        return 0

    def greet_twin(k, _):
        greet(k, twin)
        return 0

    lax.fori_loop(1, members, greet_mate, 0)
    lax.fori_loop(1, groups, greet_twin, 0)

    masks, slots = schedule(members)

    def piece(step):
        mask = 0
        for s, value in enumerate(masks):
            mask = value if s == 0 else jnp.where(step == s, value, mask)
        return partner_of(position, mask, bits)

    def loads(step):
        columns = pl.ds(pl.multiple_of(piece(step) * TILE, TILE), TILE)
        return (
            pltpu.make_async_copy(pix_ref.at[:, :, columns], pix.at[step], load_sem.at[0, step]),
            pltpu.make_async_copy(flag_ref.at[:, :, columns], flag.at[step], load_sem.at[1, step]),
        )

    def start_loads(step, _):
        for copy in loads(step):
            copy.start()
        return 0

    lax.fori_loop(0, members, start_loads, 0)

    def landing(sender):
        return out_ref.at[0, pl.ds(pl.multiple_of(sender * rows, rows), rows)]

    def delivery(step):
        return pltpu.make_async_remote_copy(
            src_ref=send.at[step],
            dst_ref=landing(position),
            send_sem=send_sem.at[step],
            recv_sem=recv_sem,
            device_id=(first + piece(step),),
            device_id_type=pl.DeviceIdType.MESH,
        )

    residue, spread, fix = lane_tables(bands)

    def work(step, totals, target):
        for copy in loads(step):
            copy.wait()
        totals = list(totals)
        for top in range(0, rows, SUBLANES):
            for left in range(0, TILE, LANES):
                spread_bands = []
                for b in range(bands):
                    x = pix[step, b, top:top + SUBLANES, left:left + LANES]
                    usable = flag[step, b, top:top + SUBLANES, left:left + LANES] == 1
                    filled = jnp.where(usable, x, 0.0)
                    low, high, count, total, squares = totals[b * STATS:(b + 1) * STATS]
                    totals[b * STATS:(b + 1) * STATS] = (
                        jnp.minimum(low, jnp.where(usable, x, largest_value)),
                        jnp.maximum(high, jnp.where(usable, x, -largest_value)),
                        count + jnp.where(usable, 1.0, 0.0),
                        total + filled,
                        squares + filled * filled,
                    )
                    spread_bands.append(permute(filled, spread[b]))
                for j in range(bands):
                    mixed = spread_bands[(bands - j) % bands]
                    for r in range(1, bands):
                        mixed = jnp.where(residue == r, spread_bands[(r - j) % bands], mixed)
                    if j:
                        mixed = permute(mixed, fix[j])
                    target(top, left * bands + j * LANES, mixed)
        return tuple(totals)

    def to_send(step):
        def put(top, left, value):
            send[step, top:top + SUBLANES, left:left + LANES] = value
        return put

    zero = jnp.zeros((SUBLANES, LANES), jnp.float32)
    totals = (zero + largest_value, zero - largest_value, zero, zero, zero) * bands
    totals = work(0, totals, to_send(0))
    pl.semaphore_wait(barrier, members - 1 + groups - 1)
    delivery(0).start()

    def work_and_send(step, totals):
        totals = work(step, totals, to_send(step))
        delivery(step).start()
        return totals

    def work_only(step, totals):
        return work(step, totals, to_send(step))

    totals = lax.fori_loop(1, early, work_and_send, totals)
    totals = lax.fori_loop(early, members - 1, work_only, totals)

    own = pl.multiple_of(position * rows, rows)

    def to_own(top, left, value):
        out_ref[0, pl.ds(own + top, SUBLANES), left:left + LANES] = value

    totals = work(members - 1, totals, to_own)

    lane = lax.broadcasted_iota(jnp.int32, (1, LANES), 1)
    line = jnp.zeros((1, LANES), jnp.float32)
    for b in range(bands):
        for s, reduce in enumerate((jnp.min, jnp.max, jnp.sum, jnp.sum, jnp.sum)):
            value = totals[b * STATS + s]
            value = reduce(reduce(value, axis=0, keepdims=True), axis=1, keepdims=True)
            line = jnp.where(lane == b * SLOT + s, value, line)
    row[0] = line
    rows_in[pl.ds(position, 1)] = line[None]

    def row_copy(k, stage, target, source):
        return pltpu.make_async_remote_copy(
            src_ref=row.at[stage],
            dst_ref=target,
            send_sem=row_send.at[stage],
            recv_sem=row_recv.at[stage],
            device_id=(source(k),),
            device_id_type=pl.DeviceIdType.MESH,
        )

    def start_row(k, _):
        row_copy(k, 0, rows_in.at[position], mate).start()
        return 0

    def start_group_row(k, _):
        row_copy(k, 1, stat_out.at[me // members], twin).start()
        return 0

    def merge_group():
        others = rows_in.at[pl.ds(0, members - 1)]
        pltpu.make_async_copy(others, others, row_recv.at[0]).wait()
        merged = merge_rows(rows_in[:, 0, :])
        row[1] = merged
        stat_out[pl.ds(me // members, 1)] = merged[None]
        lax.fori_loop(1, groups, start_group_row, 0)

    lax.fori_loop(1, members, start_row, 0)

    waited = set()
    for k, slot in enumerate(slots):
        if slot[0] < early:
            continue
        if k >= WINDOW:
            for step in slots[k - WINDOW]:
                delivery(step).wait_send()
                waited.add(step)
        for step in slot:
            delivery(step).start()
        if k == len(slots) // 2 + 1:
            merge_group()
    for step in range(members - 1):
        if step not in waited:
            delivery(step).wait_send()
    others = rows_in.at[pl.ds(0, members - 1)]
    pltpu.make_async_copy(others, others, row_send.at[0]).wait()
    if groups > 1:
        others = stat_out.at[pl.ds(0, groups - 1)]
        pltpu.make_async_copy(others, others, row_send.at[1]).wait()
        pltpu.make_async_copy(others, others, row_recv.at[1]).wait()
    arrived = out_ref.at[0, pl.ds(0, (members - 1) * rows)]
    pltpu.make_async_copy(arrived, arrived, recv_sem).wait()


def finish(bands, cell_total, chunks, tiles_ref, stats_ref, out_ref, header_ref, header, sem):
    height = tiles_ref.shape[1] // chunks
    copies = [
        pltpu.make_async_copy(
            tiles_ref.at[:, pl.ds(c * height, height)],
            out_ref.at[:, pl.ds(c * height, height)],
            sem.at[c],
        )
        for c in range(chunks)
    ]
    for copy in copies:
        copy.start()
    stats = stats_ref[:, 0, :]
    low = jnp.min(stats, axis=0, keepdims=True)
    high = jnp.max(stats, axis=0, keepdims=True)
    total = jnp.sum(stats, axis=0, keepdims=True)
    which = lax.broadcasted_iota(jnp.int32, (1, LANES), 1) % SLOT
    count = jnp.where(which == 2, total, 0.0)
    divisor = jnp.maximum(pltpu.roll(count, 1, 1) + pltpu.roll(count, 2, 1), 1.0)
    mean = total / divisor
    average = pltpu.roll(mean, 1, 1)
    deviation = jnp.sqrt(jnp.maximum(mean - average * average, 0.25))
    values = jnp.where(which == 3, mean, deviation)
    values = jnp.where(which == 2, total / cell_total, values)
    values = jnp.where(which == 1, high, values)
    values = jnp.where(which == 0, low, values)
    for b in range(bands):
        header[b:b + 1, :] = values[:, b * SLOT:b * SLOT + STATS]
    header_copy = pltpu.make_async_copy(header, header_ref, sem.at[chunks])
    header_copy.start()
    for copy in copies:
        copy.wait()
    header_copy.wait()


def on_device(pixels, valid_flags):
    bands, rows, columns = pixels.shape
    n = lax.axis_size("dev")
    members = columns // TILE
    any_space = pl.BlockSpec(memory_space=pl.ANY)
    vmem_space = pl.BlockSpec(memory_space=pltpu.VMEM)
    tiles, stats = pl.pallas_call(
        functools.partial(exchange, n, members, EARLY),
        out_shape=(
            pltpu.VMEM((1, members * rows, TILE * bands), jnp.float32),
            pltpu.VMEM((n // members, 1, LANES), jnp.float32),
        ),
        in_specs=[any_space] * 2,
        out_specs=[vmem_space] * 2,
        scratch_shapes=[
            pltpu.VMEM((members, bands, rows, TILE), jnp.float32),
            pltpu.VMEM((members, bands, rows, TILE), jnp.int32),
            pltpu.VMEM((members - 1, rows, TILE * bands), jnp.float32),
            pltpu.VMEM((2, 1, LANES), jnp.float32),
            pltpu.VMEM((members, 1, LANES), jnp.float32),
            pltpu.SemaphoreType.DMA((2, members)),
            pltpu.SemaphoreType.DMA((members - 1,)),
            pltpu.SemaphoreType.DMA,
            pltpu.SemaphoreType.DMA((2,)),
            pltpu.SemaphoreType.DMA((2,)),
        ],
        compiler_params=pltpu.CompilerParams(collective_id=0, has_side_effects=True),
        name="exchange",
    )(pixels, valid_flags)
    chunks = 4
    tiles = pltpu.with_memory_space_constraint(tiles, pltpu.VMEM)
    stats = pltpu.with_memory_space_constraint(stats, pltpu.VMEM)
    out, header = pl.pallas_call(
        functools.partial(finish, bands, rows * columns * n, chunks),
        out_shape=(
            jax.ShapeDtypeStruct(tiles.shape, jnp.float32),
            jax.ShapeDtypeStruct((bands, STATS), jnp.float32),
        ),
        in_specs=[vmem_space] * 2,
        out_specs=[any_space, any_space],
        scratch_shapes=[
            pltpu.VMEM((bands, STATS), jnp.float32),
            pltpu.SemaphoreType.DMA((chunks + 1,)),
        ],
        name="finish",
    )(tiles, stats)
    return out, header.T


def solution(mesh):
    in_specs = (P(None, "dev", None), P(None, "dev", None))
    out_specs = (P("dev", None, None), P())
    return jax.shard_map(
        on_device, mesh=mesh, in_specs=in_specs, out_specs=out_specs, check_vma=False
    )
```

```python
import functools

import jax
import jax.numpy as jnp
from jax import lax
from jax.experimental import pallas as pl
from jax.experimental.pallas import tpu as pltpu
from jax.sharding import PartitionSpec as P

TILE = 512
LANES = 128
SUBLANES = 8
STATS = 5
SLOT = 8
WINDOW = 3
AHEAD = (0, 4)

largest_value = 3e38


def schedule(members):
    dims = members.bit_length() - 2
    whole = members // 2 - 1
    near = [1 << dim for dim in range(dims)]
    turns = {}
    for dim in range(dims):
        after = (dim + 1) % dims
        turns.setdefault((1 << dim) + (1 << after), (dim, after))
    relayed = [high for high in turns if high.bit_count() == 2 and high != whole]
    paired = sorted((high for high in range(1, whole) if high > whole - high),
                    key=lambda high: (-max(high.bit_count(), (whole - high).bit_count()), high))
    left = [high for high in range(1, whole) if high.bit_count() > 1 and high not in relayed]
    groups = [[(high, 0) for high in relayed], [(high, 0) for high in near], [(whole, 1)], [(whole, 0)]]
    groups += [[(whole - high, 1), (high, 1)] for high in paired]
    groups += [[(high, 0)] for high in left]
    groups[4].append((0, 1))
    masks, slots = [], []
    for group in groups:
        slots.append(list(range(len(masks), len(masks) + len(group))))
        masks += [high * 2 + core for high, core in group]
    return masks + [0], slots, [turns[high] for high in relayed]


def lane_tables(bands):
    block = LANES // bands
    lane = lax.broadcasted_iota(jnp.int32, (SUBLANES, LANES), 1)
    m, r = lane // bands, lane % bands
    spread = [(r - b + bands) % bands * block + m for b in range(bands)]
    fix = [m * bands + (r + j) % bands for j in range(bands)]
    return r, spread, fix


def permute(x, index):
    return jnp.take_along_axis(x, index, axis=1, mode="promise_in_bounds")


def merge_rows(stats):
    which = lax.broadcasted_iota(jnp.int32, (1, LANES), 1) % SLOT
    low = jnp.min(stats, axis=0, keepdims=True)
    high = jnp.max(stats, axis=0, keepdims=True)
    total = jnp.sum(stats, axis=0, keepdims=True)
    return jnp.where(which == 0, low, jnp.where(which == 1, high, total))


def exchange(n, members, pix_ref, flag_ref, out_ref, stat_out, pix, flag, send, row, rows_in,
             relay, load_sem, send_sem, relay_send, relay_recv, recv_sem, row_send, row_recv, reach, cross):
    bands, rows, _ = pix_ref.shape
    bits = members.bit_length() - 1
    groups = n // members
    me = lax.axis_index("dev")
    position = me % members
    first = me - position
    keeper = members - 1
    turns = [(1 - 2 * (position // (1 << bit) % 2)) * (1 << bit) for bit in range(bits)]
    masks, slots, bends = schedule(members)
    lead, soon = slots[0], slots[1]

    def peer(mask):
        where = position
        for bit in range(bits):
            if mask >> bit & 1:
                where = where + turns[bit]
        return where

    def mate(k):
        return first + (position + k) % members

    def twin(k):
        return (me + k * members) % n

    def signal(semaphore, whom):
        pl.semaphore_signal(semaphore, inc=1, device_id=(whom,),
                            device_id_type=pl.DeviceIdType.MESH)

    def loads(step, where):
        columns = pl.ds(pl.multiple_of(where * TILE, TILE), TILE)
        return (
            pltpu.make_async_copy(pix_ref.at[:, :, columns], pix.at[step], load_sem.at[0, step]),
            pltpu.make_async_copy(flag_ref.at[:, :, columns], flag.at[step], load_sem.at[1, step]),
        )

    def start_loads(steps):
        for step in steps:
            for copy in loads(step, peer(masks[step])):
                copy.start()

    start_loads(lead)

    def each(lo, hi, act):
        def body(k, _):
            act(k)
            return 0

        lax.fori_loop(lo, hi, body, 0)

    barrier = pltpu.get_barrier_semaphore()
    close = [1] + [(1 << bit) + core for bit in range(1, bits) for core in (0, 1)]
    for mask in close:
        signal(barrier, first + peer(mask))

    @pl.when(position == keeper)
    def _():
        each(1, groups, lambda k: signal(barrier, twin(k)))

    start_loads(range(len(lead), members))

    def widen(level):
        for bit in range(1, bits):
            signal(reach.at[level], first + peer(1 << bit))

    def copy_to(source, target, send_to, receive, mask):
        return pltpu.make_async_remote_copy(
            src_ref=source,
            dst_ref=target,
            send_sem=send_to,
            recv_sem=receive,
            device_id=(first + peer(mask),),
            device_id_type=pl.DeviceIdType.MESH,
        )

    def landing(sender):
        return out_ref.at[0, pl.ds(pl.multiple_of(sender * rows, rows), rows)]

    def outbound(step, top=0, height=rows):
        return copy_to(
            send.at[step, pl.ds(top, height)], relay.at[step, pl.ds(top, height)],
            send_sem.at[step], relay_recv.at[step], 2 << bends[step][0],
        )

    def forward(step):
        start, after = bends[step]
        return copy_to(
            relay.at[step], landing(peer(2 << start)), relay_send.at[step], recv_sem, 2 << after
        )

    def delivery(step):
        if step in lead:
            return outbound(step)
        return copy_to(send.at[step], landing(position), send_sem.at[step], recv_sem, masks[step])

    residue, spread, fix = lane_tables(bands)

    def wait_loads(step):
        for copy in loads(step, 0):
            copy.wait()

    def work(step, tops, totals, target):
        totals = list(totals)
        for top in tops:
            for left in range(0, TILE, LANES):
                spread_bands = []
                for b in range(bands):
                    x = pix[step, b, top:top + SUBLANES, left:left + LANES]
                    usable = flag[step, b, top:top + SUBLANES, left:left + LANES] == 1
                    filled = jnp.where(usable, x, 0.0)
                    low, high, count, total, squares = totals[b * STATS:(b + 1) * STATS]
                    totals[b * STATS:(b + 1) * STATS] = (
                        jnp.minimum(low, jnp.where(usable, x, largest_value)),
                        jnp.maximum(high, jnp.where(usable, x, -largest_value)),
                        count + jnp.where(usable, 1.0, 0.0),
                        total + filled,
                        squares + filled * filled,
                    )
                    spread_bands.append(permute(filled, spread[b]))
                for j in range(bands):
                    mixed = spread_bands[(bands - j) % bands]
                    for r in range(1, bands):
                        mixed = jnp.where(residue == r, spread_bands[(r - j) % bands], mixed)
                    if j:
                        mixed = permute(mixed, fix[j])
                    target(top, left * bands + j * LANES, mixed)
        return tuple(totals)

    def to_send(step):
        def put(top, left, value):
            send[step, top:top + SUBLANES, left:left + LANES] = value
        return put

    tops = range(0, rows, SUBLANES)

    def work_only(step, totals):
        wait_loads(step)
        return work(step, tops, totals, to_send(step))

    zero = jnp.zeros((SUBLANES, LANES), jnp.float32)
    totals = (zero + largest_value, zero - largest_value, zero, zero, zero) * bands
    for top in tops:
        for step in lead:
            if top == 0:
                wait_loads(step)
            totals = work(step, (top,), totals, to_send(step))
            if top == 0 and step == 0:
                pl.semaphore_wait(barrier, len(close) + jnp.where(position == keeper, groups - 1, 0))
                widen(0)
            outbound(step, top, SUBLANES).start()
    done = len(lead)
    for step in soon:
        totals = work_only(step, totals)
        delivery(step).start()
        done += 1

    for level in range(bits - 2):
        totals = lax.fori_loop(done, done + AHEAD[level], work_only, totals)
        done += AHEAD[level]
        pl.semaphore_wait(reach.at[level], bits - 1)
        if level < bits - 3:
            widen(level + 1)

    @pl.when(position == keeper)
    def _():
        each(1, groups, lambda k: signal(cross, twin(k)))

    for step in slots[2]:
        delivery(step).start()
    totals = lax.fori_loop(done, members - 1, work_only, totals)

    own = pl.multiple_of(position * rows, rows)

    def to_own(top, left, value):
        out_ref[0, pl.ds(own + top, SUBLANES), left:left + LANES] = value

    wait_loads(members - 1)
    totals = work(members - 1, tops, totals, to_own)

    lane = lax.broadcasted_iota(jnp.int32, (1, LANES), 1)
    line = jnp.zeros((1, LANES), jnp.float32)
    for b in range(bands):
        for s, reduce in enumerate((jnp.min, jnp.max, jnp.sum, jnp.sum, jnp.sum)):
            value = totals[b * STATS + s]
            value = reduce(reduce(value, axis=0, keepdims=True), axis=1, keepdims=True)
            line = jnp.where(lane == b * SLOT + s, value, line)
    row[0] = line
    rows_in[keeper] = line

    group = me // members

    def row_copy(source, target, stage, whom):
        return pltpu.make_async_remote_copy(
            src_ref=source,
            dst_ref=target,
            send_sem=row_send.at[stage],
            recv_sem=row_recv.at[stage],
            device_id=(whom,),
            device_id_type=pl.DeviceIdType.MESH,
        )

    def to_keeper():
        return row_copy(row.at[0], rows_in.at[position], 0, first + keeper)

    def to_other(k):
        return row_copy(row.at[1], stat_out.at[group], 1, (me + k) % n)

    @pl.when(position != keeper)
    def _():
        to_keeper().start()

    def share():
        others = rows_in.at[pl.ds(0, members - 1)]
        pltpu.make_async_copy(others, others, row_recv.at[0]).wait()
        merged = merge_rows(rows_in[0:members, 0, :])
        row[1] = merged
        stat_out[pl.ds(group, 1)] = merged[None]
        if groups > 1:
            pl.semaphore_wait(cross, groups - 1)
        each(1, n, lambda k: to_other(k).start())

    sends = [[delivery(step) for step in slot] for slot in slots]
    sends.insert(3, [forward(step) for step in lead])
    started, waited = 3, 0
    for k in range(started, len(sends)):
        for copy in sends[k - WINDOW]:
            copy.wait_send()
        if k == 3:
            for step in lead:
                outbound(step).wait_recv()
        for copy in sends[k]:
            copy.start()
        if k == len(sends) - 2:
            pl.when(position == keeper)(share)
    for k in range(len(sends) - WINDOW, len(sends)):
        for copy in sends[k]:
            copy.wait_send()

    @pl.when(position == keeper)
    def _():
        sent = rows_in.at[pl.ds(0, n - 1)]
        pltpu.make_async_copy(sent, sent, row_send.at[1]).wait()
        if groups > 1:
            others = stat_out.at[pl.ds(0, groups - 1)]
            pltpu.make_async_copy(others, others, row_recv.at[1]).wait()

    @pl.when(position != keeper)
    def _():
        to_keeper().wait_send()
        pltpu.make_async_copy(stat_out, stat_out, row_recv.at[1]).wait()

    arrived = out_ref.at[0, pl.ds(0, (members - 1) * rows)]
    pltpu.make_async_copy(arrived, arrived, recv_sem).wait()


def finish(bands, cell_total, chunks, tiles_ref, stats_ref, out_ref, header_ref, header, sem):
    height = tiles_ref.shape[1] // chunks
    copies = [
        pltpu.make_async_copy(
            tiles_ref.at[:, pl.ds(c * height, height)],
            out_ref.at[:, pl.ds(c * height, height)],
            sem.at[c],
        )
        for c in range(chunks)
    ]
    for copy in copies:
        copy.start()
    stats = stats_ref[:, 0, :]
    low = jnp.min(stats, axis=0, keepdims=True)
    high = jnp.max(stats, axis=0, keepdims=True)
    total = jnp.sum(stats, axis=0, keepdims=True)
    which = lax.broadcasted_iota(jnp.int32, (1, LANES), 1) % SLOT
    count = jnp.where(which == 2, total, 0.0)
    divisor = jnp.maximum(pltpu.roll(count, 1, 1) + pltpu.roll(count, 2, 1), 1.0)
    mean = total / divisor
    average = pltpu.roll(mean, 1, 1)
    deviation = jnp.sqrt(jnp.maximum(mean - average * average, 0.25))
    values = jnp.where(which == 3, mean, deviation)
    values = jnp.where(which == 2, total / cell_total, values)
    values = jnp.where(which == 1, high, values)
    values = jnp.where(which == 0, low, values)
    for b in range(bands):
        header[b:b + 1, :] = values[:, b * SLOT:b * SLOT + STATS]
    header_copy = pltpu.make_async_copy(header, header_ref, sem.at[chunks])
    header_copy.start()
    for copy in copies:
        copy.wait()
    header_copy.wait()


def on_device(pixels, valid_flags):
    bands, rows, columns = pixels.shape
    n = lax.axis_size("dev")
    members = columns // TILE
    relays = len(schedule(members)[2])
    any_space = pl.BlockSpec(memory_space=pl.ANY)
    vmem_space = pl.BlockSpec(memory_space=pltpu.VMEM)
    tiles, stats = pl.pallas_call(
        functools.partial(exchange, n, members),
        out_shape=(
            pltpu.VMEM((1, members * rows, TILE * bands), jnp.float32),
            pltpu.VMEM((n // members, 1, LANES), jnp.float32),
        ),
        in_specs=[any_space] * 2,
        out_specs=[vmem_space] * 2,
        scratch_shapes=[
            pltpu.VMEM((members, bands, rows, TILE), jnp.float32),
            pltpu.VMEM((members, bands, rows, TILE), jnp.int32),
            pltpu.VMEM((members - 1, rows, TILE * bands), jnp.float32),
            pltpu.VMEM((2, 1, LANES), jnp.float32),
            pltpu.VMEM((n, 1, LANES), jnp.float32),
            pltpu.VMEM((relays, rows, TILE * bands), jnp.float32),
            pltpu.SemaphoreType.DMA((2, members)),
            pltpu.SemaphoreType.DMA((members - 1,)),
            pltpu.SemaphoreType.DMA((relays,)),
            pltpu.SemaphoreType.DMA((relays,)),
            pltpu.SemaphoreType.DMA,
            pltpu.SemaphoreType.DMA((2,)),
            pltpu.SemaphoreType.DMA((2,)),
            pltpu.SemaphoreType.REGULAR((members.bit_length() - 3,)),
            pltpu.SemaphoreType.REGULAR,
        ],
        compiler_params=pltpu.CompilerParams(collective_id=0, has_side_effects=True),
        name="exchange",
    )(pixels, valid_flags)
    chunks = 4
    tiles = pltpu.with_memory_space_constraint(tiles, pltpu.VMEM)
    stats = pltpu.with_memory_space_constraint(stats, pltpu.VMEM)
    out, header = pl.pallas_call(
        functools.partial(finish, bands, rows * columns * n, chunks),
        out_shape=(
            jax.ShapeDtypeStruct(tiles.shape, jnp.float32),
            jax.ShapeDtypeStruct((bands, STATS), jnp.float32),
        ),
        in_specs=[vmem_space] * 2,
        out_specs=[any_space, any_space],
        scratch_shapes=[
            pltpu.VMEM((bands, STATS), jnp.float32),
            pltpu.SemaphoreType.DMA((chunks + 1,)),
        ],
        name="finish",
    )(tiles, stats)
    return out, header.T


def solution(mesh):
    in_specs = (P(None, "dev", None), P(None, "dev", None))
    out_specs = (P("dev", None, None), P())
    return jax.shard_map(
        on_device, mesh=mesh, in_specs=in_specs, out_specs=out_specs, check_vma=False
    )
```

```python
import functools

import jax
import jax.numpy as jnp
from jax import lax
from jax.experimental import pallas as pl
from jax.experimental.pallas import tpu as pltpu
from jax.sharding import PartitionSpec as P

TILE = 512
LANES = 128
SUBLANES = 8
STATS = 5
SLOT = 8
WINDOW = 3
AHEAD = 3

largest_value = 3e38


def schedule(members):
    dims = members.bit_length() - 2
    whole = members // 2 - 1
    near = [1 << dim for dim in range(dims)]
    turns = {}
    for dim in range(dims):
        after = (dim + 1) % dims
        turns.setdefault((1 << dim) + (1 << after), (dim, after))
    relayed = [high for high in turns if high.bit_count() == 2 and high != whole]
    paired = sorted((high for high in range(1, whole) if high > whole - high),
                    key=lambda high: (-max(high.bit_count(), (whole - high).bit_count()), high))
    left = [high for high in range(1, whole) if high.bit_count() > 1 and high not in relayed]
    groups = [[(high, 0) for high in relayed], [(high, 0) for high in near], [(whole, 1)], [(whole, 0)]]
    groups += [[(whole - high, 1), (high, 1)] for high in paired]
    groups += [[(high, 0)] for high in left]
    groups[4].append((0, 1))
    masks, slots = [], []
    for group in groups:
        slots.append(list(range(len(masks), len(masks) + len(group))))
        masks += [high * 2 + core for high, core in group]
    return masks + [0], slots, [turns[high] for high in relayed]


def lane_tables(bands):
    block = LANES // bands
    lane = lax.broadcasted_iota(jnp.int32, (SUBLANES, LANES), 1)
    m, r = lane // bands, lane % bands
    spread = [(r - b + bands) % bands * block + m for b in range(bands)]
    fix = [m * bands + (r + j) % bands for j in range(bands)]
    return r, spread, fix


def permute(x, index):
    return jnp.take_along_axis(x, index, axis=1, mode="promise_in_bounds")


def merge_rows(stats):
    which = lax.broadcasted_iota(jnp.int32, (1, LANES), 1) % SLOT
    low = jnp.min(stats, axis=0, keepdims=True)
    high = jnp.max(stats, axis=0, keepdims=True)
    total = jnp.sum(stats, axis=0, keepdims=True)
    return jnp.where(which == 0, low, jnp.where(which == 1, high, total))


def exchange(n, members, pix_ref, flag_ref, out_ref, stat_out, pix, flag, send, row, rows_in,
             relay, load_sem, send_sem, relay_send, relay_recv, recv_sem, row_send, row_recv, reach, cross):
    bands, rows, _ = pix_ref.shape
    bits = members.bit_length() - 1
    groups = n // members
    me = lax.axis_index("dev")
    position = me % members
    first = me - position
    keeper = members - 1
    turns = [(1 - 2 * (position // (1 << bit) % 2)) * (1 << bit) for bit in range(bits)]
    masks, slots, bends = schedule(members)
    lead, soon = slots[0], slots[1]

    def peer(mask):
        where = position
        for bit in range(bits):
            if mask >> bit & 1:
                where = where + turns[bit]
        return where

    where = [peer(mask) for mask in masks]
    late = where[slots[-1][0]] < 2
    for step in slots[-1][1:]:
        late = jnp.logical_or(late, where[step] < 2)
    for a, b in zip(slots[-2], slots[-1]):
        where[a], where[b] = jnp.where(late, where[b], where[a]), jnp.where(late, where[a], where[b])

    def mate(k):
        return first + (position + k) % members

    def twin(k):
        return (me + k * members) % n

    def signal(semaphore, whom):
        pl.semaphore_signal(semaphore, inc=1, device_id=(whom,),
                            device_id_type=pl.DeviceIdType.MESH)

    def loads(step, where):
        columns = pl.ds(pl.multiple_of(where * TILE, TILE), TILE)
        return (
            pltpu.make_async_copy(pix_ref.at[:, :, columns], pix.at[step], load_sem.at[0, step]),
            pltpu.make_async_copy(flag_ref.at[:, :, columns], flag.at[step], load_sem.at[1, step]),
        )

    def start_loads(steps):
        for step in steps:
            for copy in loads(step, where[step]):
                copy.start()

    start_loads(lead)

    def each(lo, hi, act):
        def body(k, _):
            act(k)
            return 0

        lax.fori_loop(lo, hi, body, 0)

    barrier = pltpu.get_barrier_semaphore()
    close = [1] + [(1 << bit) + core for bit in range(1, bits) for core in (0, 1)]
    for mask in close:
        signal(barrier, first + peer(mask))

    @pl.when(position == keeper)
    def _():
        each(1, groups, lambda k: signal(barrier, twin(k)))

    start_loads(range(len(lead), members))

    def widen(level):
        for bit in range(1, bits):
            signal(reach.at[level], first + peer(1 << bit))

    def copy_to(source, target, send_to, receive, whom):
        return pltpu.make_async_remote_copy(
            src_ref=source,
            dst_ref=target,
            send_sem=send_to,
            recv_sem=receive,
            device_id=(first + whom,),
            device_id_type=pl.DeviceIdType.MESH,
        )

    def landing(sender):
        return out_ref.at[0, pl.ds(pl.multiple_of(sender * rows, rows), rows)]

    def outbound(step, top=0, height=rows):
        return copy_to(
            send.at[step, pl.ds(top, height)], relay.at[step, pl.ds(top, height)],
            send_sem.at[step], relay_recv.at[step], peer(2 << bends[step][0]),
        )

    def forward(step):
        start, after = bends[step]
        return copy_to(
            relay.at[step], landing(peer(2 << start)), relay_send.at[step], recv_sem, peer(2 << after)
        )

    def delivery(step, top=0, height=rows):
        start = pl.multiple_of(position * rows + top, SUBLANES)
        return copy_to(
            send.at[step, pl.ds(top, height)], out_ref.at[0, pl.ds(start, height)],
            send_sem.at[step], recv_sem, where[step],
        )

    half = rows // 2 // SUBLANES * SUBLANES

    residue, spread, fix = lane_tables(bands)

    def wait_loads(step):
        for copy in loads(step, 0):
            copy.wait()

    def work(step, tops, totals, target):
        totals = list(totals)
        for top in tops:
            for left in range(0, TILE, LANES):
                spread_bands = []
                for b in range(bands):
                    x = pix[step, b, top:top + SUBLANES, left:left + LANES]
                    usable = flag[step, b, top:top + SUBLANES, left:left + LANES] == 1
                    filled = jnp.where(usable, x, 0.0)
                    low, high, count, total, squares = totals[b * STATS:(b + 1) * STATS]
                    totals[b * STATS:(b + 1) * STATS] = (
                        jnp.minimum(low, jnp.where(usable, x, largest_value)),
                        jnp.maximum(high, jnp.where(usable, x, -largest_value)),
                        count + jnp.where(usable, 1.0, 0.0),
                        total + filled,
                        squares + filled * filled,
                    )
                    spread_bands.append(permute(filled, spread[b]))
                for j in range(bands):
                    mixed = spread_bands[(bands - j) % bands]
                    for r in range(1, bands):
                        mixed = jnp.where(residue == r, spread_bands[(r - j) % bands], mixed)
                    if j:
                        mixed = permute(mixed, fix[j])
                    target(top, left * bands + j * LANES, mixed)
        return tuple(totals)

    def to_send(step):
        def put(top, left, value):
            send[step, top:top + SUBLANES, left:left + LANES] = value
        return put

    tops = range(0, rows, SUBLANES)

    def work_only(step, totals):
        wait_loads(step)
        return work(step, tops, totals, to_send(step))

    zero = jnp.zeros((SUBLANES, LANES), jnp.float32)
    totals = (zero + largest_value, zero - largest_value, zero, zero, zero) * bands
    for step in lead:
        wait_loads(step)
    for top in tops:
        for step in lead:
            totals = work(step, (top,), totals, to_send(step))
        if top == 0:
            pl.semaphore_wait(barrier, len(close) + jnp.where(position == keeper, groups - 1, 0))
            widen(0)
        for step in lead:
            outbound(step, top, SUBLANES).start()
    done = len(lead)
    for level in range(bits - 2):
        pl.semaphore_wait(reach.at[level], bits - 1)
        if level < bits - 3:
            widen(level + 1)
        if level == 0:
            for step in soon:
                totals = work_only(step, totals)
                delivery(step).start()
                done += 1
            totals = lax.fori_loop(done, done + AHEAD, work_only, totals)
            done += AHEAD

    @pl.when(position == keeper)
    def _():
        each(1, groups, lambda k: signal(cross, twin(k)))

    for step in slots[2]:
        delivery(step).start()
    totals = lax.fori_loop(done, members - 1, work_only, totals)

    own = pl.multiple_of(position * rows, rows)

    def to_own(top, left, value):
        out_ref[0, pl.ds(own + top, SUBLANES), left:left + LANES] = value

    wait_loads(members - 1)
    totals = work(members - 1, tops, totals, to_own)

    lane = lax.broadcasted_iota(jnp.int32, (1, LANES), 1)
    line = jnp.zeros((1, LANES), jnp.float32)
    for b in range(bands):
        for s, reduce in enumerate((jnp.min, jnp.max, jnp.sum, jnp.sum, jnp.sum)):
            value = totals[b * STATS + s]
            value = reduce(reduce(value, axis=0, keepdims=True), axis=1, keepdims=True)
            line = jnp.where(lane == b * SLOT + s, value, line)
    row[0] = line
    rows_in[keeper] = line

    group = me // members

    def row_copy(source, target, stage, whom):
        return pltpu.make_async_remote_copy(
            src_ref=source,
            dst_ref=target,
            send_sem=row_send.at[stage],
            recv_sem=row_recv.at[stage],
            device_id=(whom,),
            device_id_type=pl.DeviceIdType.MESH,
        )

    def to_keeper():
        return row_copy(row.at[0], rows_in.at[position], 0, first + keeper)

    def to_other(k):
        return row_copy(row.at[1], stat_out.at[group], 1, (me + k) % n)

    @pl.when(position != keeper)
    def _():
        to_keeper().start()

    def share():
        others = rows_in.at[pl.ds(0, members - 1)]
        pltpu.make_async_copy(others, others, row_recv.at[0]).wait()
        merged = merge_rows(rows_in[0:members, 0, :])
        row[1] = merged
        stat_out[pl.ds(group, 1)] = merged[None]
        if groups > 1:
            pl.semaphore_wait(cross, groups - 1)
        each(1, n, lambda k: to_other(k).start())

    sends = [
        [outbound(step) for step in lead],
        [delivery(step) for step in soon],
        [delivery(step) for step in slots[2]],
        [forward(step) for step in lead],
        *([delivery(step) for step in slot] for slot in slots[3:]),
    ]
    started = 3
    for k in range(started, len(sends)):
        for copy in sends[k - WINDOW] if k >= WINDOW else ():
            copy.wait_send()
        if k == 3:
            for step in lead:
                outbound(step).wait_recv()
        for copy in sends[k]:
            copy.start()
        if k == 5:
            pl.when(position == keeper)(share)
    for k in range(len(sends) - WINDOW, len(sends)):
        for copy in sends[k]:
            copy.wait_send()

    @pl.when(position == keeper)
    def _():
        sent = rows_in.at[pl.ds(0, n - 1)]
        pltpu.make_async_copy(sent, sent, row_send.at[1]).wait()
        if groups > 1:
            others = stat_out.at[pl.ds(0, groups - 1)]
            pltpu.make_async_copy(others, others, row_recv.at[1]).wait()

    @pl.when(position != keeper)
    def _():
        to_keeper().wait_send()
        pltpu.make_async_copy(stat_out, stat_out, row_recv.at[1]).wait()

    arrived = out_ref.at[0, pl.ds(0, (members - 1) * rows)]
    pltpu.make_async_copy(arrived, arrived, recv_sem).wait()


def finish(bands, cell_total, chunks, tiles_ref, stats_ref, out_ref, header_ref, header, sem):
    height = tiles_ref.shape[1] // chunks
    copies = [
        pltpu.make_async_copy(
            tiles_ref.at[:, pl.ds(c * height, height)],
            out_ref.at[:, pl.ds(c * height, height)],
            sem.at[c],
        )
        for c in range(chunks)
    ]
    for copy in copies:
        copy.start()
    stats = stats_ref[:, 0, :]
    low = jnp.min(stats, axis=0, keepdims=True)
    high = jnp.max(stats, axis=0, keepdims=True)
    total = jnp.sum(stats, axis=0, keepdims=True)
    which = lax.broadcasted_iota(jnp.int32, (1, LANES), 1) % SLOT
    count = jnp.where(which == 2, total, 0.0)
    divisor = jnp.maximum(pltpu.roll(count, 1, 1) + pltpu.roll(count, 2, 1), 1.0)
    mean = total / divisor
    average = pltpu.roll(mean, 1, 1)
    deviation = jnp.sqrt(jnp.maximum(mean - average * average, 0.25))
    values = jnp.where(which == 3, mean, deviation)
    values = jnp.where(which == 2, total / cell_total, values)
    values = jnp.where(which == 1, high, values)
    values = jnp.where(which == 0, low, values)
    for b in range(bands):
        header[b:b + 1, :] = values[:, b * SLOT:b * SLOT + STATS]
    header_copy = pltpu.make_async_copy(header, header_ref, sem.at[chunks])
    header_copy.start()
    for copy in copies:
        copy.wait()
    header_copy.wait()


def on_device(pixels, valid_flags):
    bands, rows, columns = pixels.shape
    n = lax.axis_size("dev")
    members = columns // TILE
    relays = len(schedule(members)[2])
    any_space = pl.BlockSpec(memory_space=pl.ANY)
    vmem_space = pl.BlockSpec(memory_space=pltpu.VMEM)
    tiles, stats = pl.pallas_call(
        functools.partial(exchange, n, members),
        out_shape=(
            pltpu.VMEM((1, members * rows, TILE * bands), jnp.float32),
            pltpu.VMEM((n // members, 1, LANES), jnp.float32),
        ),
        in_specs=[any_space] * 2,
        out_specs=[vmem_space] * 2,
        scratch_shapes=[
            pltpu.VMEM((members, bands, rows, TILE), jnp.float32),
            pltpu.VMEM((members, bands, rows, TILE), jnp.int32),
            pltpu.VMEM((members - 1, rows, TILE * bands), jnp.float32),
            pltpu.VMEM((2, 1, LANES), jnp.float32),
            pltpu.VMEM((n, 1, LANES), jnp.float32),
            pltpu.VMEM((relays, rows, TILE * bands), jnp.float32),
            pltpu.SemaphoreType.DMA((2, members)),
            pltpu.SemaphoreType.DMA((members - 1,)),
            pltpu.SemaphoreType.DMA((relays,)),
            pltpu.SemaphoreType.DMA((relays,)),
            pltpu.SemaphoreType.DMA,
            pltpu.SemaphoreType.DMA((2,)),
            pltpu.SemaphoreType.DMA((2,)),
            pltpu.SemaphoreType.REGULAR((members.bit_length() - 3,)),
            pltpu.SemaphoreType.REGULAR,
        ],
        compiler_params=pltpu.CompilerParams(collective_id=0, has_side_effects=True),
        name="exchange",
    )(pixels, valid_flags)
    chunks = 4
    tiles = pltpu.with_memory_space_constraint(tiles, pltpu.VMEM)
    stats = pltpu.with_memory_space_constraint(stats, pltpu.VMEM)
    out, header = pl.pallas_call(
        functools.partial(finish, bands, rows * columns * n, chunks),
        out_shape=(
            jax.ShapeDtypeStruct(tiles.shape, jnp.float32),
            jax.ShapeDtypeStruct((bands, STATS), jnp.float32),
        ),
        in_specs=[vmem_space] * 2,
        out_specs=[any_space, any_space],
        scratch_shapes=[
            pltpu.VMEM((bands, STATS), jnp.float32),
            pltpu.SemaphoreType.DMA((chunks + 1,)),
        ],
        name="finish",
    )(tiles, stats)
    return out, header.T


def solution(mesh):
    in_specs = (P(None, "dev", None), P(None, "dev", None))
    out_specs = (P("dev", None, None), P())
    return jax.shard_map(
        on_device, mesh=mesh, in_specs=in_specs, out_specs=out_specs, check_vma=False
    )
```

```python
import functools

import jax
import jax.numpy as jnp
from jax import lax
from jax.experimental import pallas as pl
from jax.experimental.pallas import tpu as pltpu
from jax.sharding import PartitionSpec as P

TILE = 512
LANES = 128
SUBLANES = 8
STATS = 5
SLOT = 8
WINDOW = 3
AHEAD = 3

largest_value = 3e38


def schedule(members):
    dims = members.bit_length() - 2
    whole = members // 2 - 1
    near = [1 << dim for dim in range(dims)]
    turns = {}
    for dim in range(dims):
        after = (dim + 1) % dims
        turns.setdefault((1 << dim) + (1 << after), (dim, after))
    relayed = [high for high in turns if high.bit_count() == 2 and high != whole]
    paired = sorted((high for high in range(1, whole) if high > whole - high),
                    key=lambda high: (-max(high.bit_count(), (whole - high).bit_count()), high))
    left = [high for high in range(1, whole) if high.bit_count() > 1 and high not in relayed]
    groups = [[(high, 0) for high in relayed], [(high, 0) for high in near], [(whole, 1)], [(whole, 0)]]
    groups += [[(whole - high, 1), (high, 1)] for high in paired]
    groups += [[(high, 0)] for high in left]
    groups[4].append((0, 1))
    masks, slots = [], []
    for group in groups:
        slots.append(list(range(len(masks), len(masks) + len(group))))
        masks += [high * 2 + core for high, core in group]
    return masks + [0], slots, [turns[high] for high in relayed]


def lane_tables(bands):
    block = LANES // bands
    lane = lax.broadcasted_iota(jnp.int32, (SUBLANES, LANES), 1)
    m, r = lane // bands, lane % bands
    spread = [(r - b + bands) % bands * block + m for b in range(bands)]
    fix = [m * bands + (r + j) % bands for j in range(bands)]
    return r, spread, fix


def permute(x, index):
    return jnp.take_along_axis(x, index, axis=1, mode="promise_in_bounds")


def merge_rows(stats):
    which = lax.broadcasted_iota(jnp.int32, (1, LANES), 1) % SLOT
    low = jnp.min(stats, axis=0, keepdims=True)
    high = jnp.max(stats, axis=0, keepdims=True)
    total = jnp.sum(stats, axis=0, keepdims=True)
    return jnp.where(which == 0, low, jnp.where(which == 1, high, total))


def exchange(n, members, pix_ref, flag_ref, out_ref, stat_out, pix, flag, send, row, rows_in,
             relay, load_sem, send_sem, relay_send, relay_recv, recv_sem, row_send, row_recv, reach, cross):
    bands, rows, _ = pix_ref.shape
    bits = members.bit_length() - 1
    groups = n // members
    me = lax.axis_index("dev")
    position = me % members
    first = me - position
    keeper = 1
    turns = [(1 - 2 * (position // (1 << bit) % 2)) * (1 << bit) for bit in range(bits)]
    masks, slots, bends = schedule(members)
    lead, soon = slots[0], slots[1]

    def peer(mask):
        where = position
        for bit in range(bits):
            if mask >> bit & 1:
                where = where + turns[bit]
        return where

    where = [peer(mask) for mask in masks]
    late = where[slots[-1][0]] < 2
    for step in slots[-1][1:]:
        late = jnp.logical_or(late, where[step] < 2)
    for a, b in zip(slots[-2], slots[-1]):
        where[a], where[b] = jnp.where(late, where[b], where[a]), jnp.where(late, where[a], where[b])

    def mate(k):
        return first + (position + k) % members

    def twin(k):
        return (me + k * members) % n

    def signal(semaphore, whom):
        pl.semaphore_signal(semaphore, inc=1, device_id=(whom,),
                            device_id_type=pl.DeviceIdType.MESH)

    def loads(step, where):
        columns = pl.ds(pl.multiple_of(where * TILE, TILE), TILE)
        return (
            pltpu.make_async_copy(pix_ref.at[:, :, columns], pix.at[step], load_sem.at[0, step]),
            pltpu.make_async_copy(flag_ref.at[:, :, columns], flag.at[step], load_sem.at[1, step]),
        )

    def start_loads(steps):
        for step in steps:
            for copy in loads(step, where[step]):
                copy.start()

    start_loads(lead)

    def each(lo, hi, act):
        def body(k, _):
            act(k)
            return 0

        lax.fori_loop(lo, hi, body, 0)

    barrier = pltpu.get_barrier_semaphore()
    close = [1] + [(1 << bit) + core for bit in range(1, bits) for core in (0, 1)]
    for mask in close:
        signal(barrier, first + peer(mask))

    @pl.when(position == keeper)
    def _():
        each(1, groups, lambda k: signal(barrier, twin(k)))

    start_loads(range(len(lead), members))

    def widen(level):
        for bit in range(1, bits):
            signal(reach.at[level], first + peer(1 << bit))

    def copy_to(source, target, send_to, receive, whom):
        return pltpu.make_async_remote_copy(
            src_ref=source,
            dst_ref=target,
            send_sem=send_to,
            recv_sem=receive,
            device_id=(first + whom,),
            device_id_type=pl.DeviceIdType.MESH,
        )

    def landing(sender):
        return out_ref.at[0, pl.ds(pl.multiple_of(sender * rows, rows), rows)]

    def outbound(step, top=0, height=rows):
        return copy_to(
            send.at[step, pl.ds(top, height)], relay.at[step, pl.ds(top, height)],
            send_sem.at[step], relay_recv.at[step], peer(2 << bends[step][0]),
        )

    def forward(step):
        start, after = bends[step]
        return copy_to(
            relay.at[step], landing(peer(2 << start)), relay_send.at[step], recv_sem, peer(2 << after)
        )

    def delivery(step, top=0, height=rows):
        start = pl.multiple_of(position * rows + top, SUBLANES)
        return copy_to(
            send.at[step, pl.ds(top, height)], out_ref.at[0, pl.ds(start, height)],
            send_sem.at[step], recv_sem, where[step],
        )

    half = rows // 2 // SUBLANES * SUBLANES

    residue, spread, fix = lane_tables(bands)

    def wait_loads(step):
        for copy in loads(step, 0):
            copy.wait()

    def work(step, tops, totals, target):
        totals = list(totals)
        for top in tops:
            for left in range(0, TILE, LANES):
                spread_bands = []
                for b in range(bands):
                    x = pix[step, b, top:top + SUBLANES, left:left + LANES]
                    usable = flag[step, b, top:top + SUBLANES, left:left + LANES] == 1
                    filled = jnp.where(usable, x, 0.0)
                    low, high, count, total, squares = totals[b * STATS:(b + 1) * STATS]
                    totals[b * STATS:(b + 1) * STATS] = (
                        jnp.minimum(low, jnp.where(usable, x, largest_value)),
                        jnp.maximum(high, jnp.where(usable, x, -largest_value)),
                        count + jnp.where(usable, 1.0, 0.0),
                        total + filled,
                        squares + filled * filled,
                    )
                    spread_bands.append(permute(filled, spread[b]))
                for j in range(bands):
                    mixed = spread_bands[(bands - j) % bands]
                    for r in range(1, bands):
                        mixed = jnp.where(residue == r, spread_bands[(r - j) % bands], mixed)
                    if j:
                        mixed = permute(mixed, fix[j])
                    target(top, left * bands + j * LANES, mixed)
        return tuple(totals)

    def to_send(step):
        def put(top, left, value):
            send[step, top:top + SUBLANES, left:left + LANES] = value
        return put

    tops = range(0, rows, SUBLANES)

    def work_only(step, totals):
        wait_loads(step)
        return work(step, tops, totals, to_send(step))

    zero = jnp.zeros((SUBLANES, LANES), jnp.float32)
    totals = (zero + largest_value, zero - largest_value, zero, zero, zero) * bands
    for step in lead:
        wait_loads(step)
    for top in tops:
        for step in lead:
            totals = work(step, (top,), totals, to_send(step))
        if top == 0:
            pl.semaphore_wait(barrier, len(close) + jnp.where(position == keeper, groups - 1, 0))
            widen(0)
        for step in lead:
            outbound(step, top, SUBLANES).start()
    done = len(lead)
    for level in range(bits - 2):
        pl.semaphore_wait(reach.at[level], bits - 1)
        if level < bits - 3:
            widen(level + 1)
        if level == 0:
            for step in soon:
                totals = work_only(step, totals)
                delivery(step).start()
                done += 1
            totals = lax.fori_loop(done, done + AHEAD, work_only, totals)
            done += AHEAD

    @pl.when(position == keeper)
    def _():
        each(1, groups, lambda k: signal(cross, twin(k)))

    for step in slots[2]:
        delivery(step).start()
    totals = lax.fori_loop(done, members - 1, work_only, totals)

    own = pl.multiple_of(position * rows, rows)

    def to_own(top, left, value):
        out_ref[0, pl.ds(own + top, SUBLANES), left:left + LANES] = value

    wait_loads(members - 1)
    totals = work(members - 1, tops, totals, to_own)

    lane = lax.broadcasted_iota(jnp.int32, (1, LANES), 1)
    line = jnp.zeros((1, LANES), jnp.float32)
    for b in range(bands):
        for s, reduce in enumerate((jnp.min, jnp.max, jnp.sum, jnp.sum, jnp.sum)):
            value = totals[b * STATS + s]
            value = reduce(reduce(value, axis=0, keepdims=True), axis=1, keepdims=True)
            line = jnp.where(lane == b * SLOT + s, value, line)
    row[0] = line
    rows_in[members - 1] = line

    group = me // members

    def row_copy(source, target, stage, whom):
        return pltpu.make_async_remote_copy(
            src_ref=source,
            dst_ref=target,
            send_sem=row_send.at[stage],
            recv_sem=row_recv.at[stage],
            device_id=(whom,),
            device_id_type=pl.DeviceIdType.MESH,
        )

    def to_keeper():
        return row_copy(row.at[0], rows_in.at[(position - keeper + members - 1) % members], 0, first + keeper)

    def to_other(k):
        return row_copy(row.at[1], stat_out.at[group], 1, (me + k) % n)

    @pl.when(position != keeper)
    def _():
        to_keeper().start()

    def share():
        others = rows_in.at[pl.ds(0, members - 1)]
        pltpu.make_async_copy(others, others, row_recv.at[0]).wait()
        merged = merge_rows(rows_in[0:members, 0, :])
        row[1] = merged
        stat_out[pl.ds(group, 1)] = merged[None]
        if groups > 1:
            pl.semaphore_wait(cross, groups - 1)
        each(1, n, lambda k: to_other(k).start())

    sends = [
        [outbound(step) for step in lead],
        [delivery(step) for step in soon],
        [delivery(step) for step in slots[2]],
        [forward(step) for step in lead],
        *([delivery(step) for step in slot] for slot in slots[3:]),
    ]
    started = 3
    for k in range(started, len(sends)):
        for copy in sends[k - WINDOW] if k >= WINDOW else ():
            copy.wait_send()
        if k == 3:
            for step in lead:
                outbound(step).wait_recv()
        for copy in sends[k]:
            copy.start()
        if k == 5:
            pl.when(position == keeper)(share)
    for k in range(len(sends) - WINDOW, len(sends)):
        for copy in sends[k]:
            copy.wait_send()

    @pl.when(position == keeper)
    def _():
        sent = rows_in.at[pl.ds(0, n - 1)]
        pltpu.make_async_copy(sent, sent, row_send.at[1]).wait()
        if groups > 1:
            others = stat_out.at[pl.ds(0, groups - 1)]
            pltpu.make_async_copy(others, others, row_recv.at[1]).wait()

    @pl.when(position != keeper)
    def _():
        to_keeper().wait_send()
        pltpu.make_async_copy(stat_out, stat_out, row_recv.at[1]).wait()

    arrived = out_ref.at[0, pl.ds(0, (members - 1) * rows)]
    pltpu.make_async_copy(arrived, arrived, recv_sem).wait()


def finish(bands, cell_total, chunks, tiles_ref, stats_ref, out_ref, header_ref, header, sem):
    height = tiles_ref.shape[1] // chunks
    copies = [
        pltpu.make_async_copy(
            tiles_ref.at[:, pl.ds(c * height, height)],
            out_ref.at[:, pl.ds(c * height, height)],
            sem.at[c],
        )
        for c in range(chunks)
    ]
    for copy in copies:
        copy.start()
    stats = stats_ref[:, 0, :]
    low = jnp.min(stats, axis=0, keepdims=True)
    high = jnp.max(stats, axis=0, keepdims=True)
    total = jnp.sum(stats, axis=0, keepdims=True)
    which = lax.broadcasted_iota(jnp.int32, (1, LANES), 1) % SLOT
    count = jnp.where(which == 2, total, 0.0)
    divisor = jnp.maximum(pltpu.roll(count, 1, 1) + pltpu.roll(count, 2, 1), 1.0)
    mean = total / divisor
    average = pltpu.roll(mean, 1, 1)
    deviation = jnp.sqrt(jnp.maximum(mean - average * average, 0.25))
    values = jnp.where(which == 3, mean, deviation)
    values = jnp.where(which == 2, total / cell_total, values)
    values = jnp.where(which == 1, high, values)
    values = jnp.where(which == 0, low, values)
    for b in range(bands):
        header[b:b + 1, :] = values[:, b * SLOT:b * SLOT + STATS]
    header_copy = pltpu.make_async_copy(header, header_ref, sem.at[chunks])
    header_copy.start()
    for copy in copies:
        copy.wait()
    header_copy.wait()


def on_device(pixels, valid_flags):
    bands, rows, columns = pixels.shape
    n = lax.axis_size("dev")
    members = columns // TILE
    relays = len(schedule(members)[2])
    any_space = pl.BlockSpec(memory_space=pl.ANY)
    vmem_space = pl.BlockSpec(memory_space=pltpu.VMEM)
    tiles, stats = pl.pallas_call(
        functools.partial(exchange, n, members),
        out_shape=(
            pltpu.VMEM((1, members * rows, TILE * bands), jnp.float32),
            pltpu.VMEM((n // members, 1, LANES), jnp.float32),
        ),
        in_specs=[any_space] * 2,
        out_specs=[vmem_space] * 2,
        scratch_shapes=[
            pltpu.VMEM((members, bands, rows, TILE), jnp.float32),
            pltpu.VMEM((members, bands, rows, TILE), jnp.int32),
            pltpu.VMEM((members - 1, rows, TILE * bands), jnp.float32),
            pltpu.VMEM((2, 1, LANES), jnp.float32),
            pltpu.VMEM((n, 1, LANES), jnp.float32),
            pltpu.VMEM((relays, rows, TILE * bands), jnp.float32),
            pltpu.SemaphoreType.DMA((2, members)),
            pltpu.SemaphoreType.DMA((members - 1,)),
            pltpu.SemaphoreType.DMA((relays,)),
            pltpu.SemaphoreType.DMA((relays,)),
            pltpu.SemaphoreType.DMA,
            pltpu.SemaphoreType.DMA((2,)),
            pltpu.SemaphoreType.DMA((2,)),
            pltpu.SemaphoreType.REGULAR((members.bit_length() - 3,)),
            pltpu.SemaphoreType.REGULAR,
        ],
        compiler_params=pltpu.CompilerParams(collective_id=0, has_side_effects=True),
        name="exchange",
    )(pixels, valid_flags)
    chunks = 4
    tiles = pltpu.with_memory_space_constraint(tiles, pltpu.VMEM)
    stats = pltpu.with_memory_space_constraint(stats, pltpu.VMEM)
    out, header = pl.pallas_call(
        functools.partial(finish, bands, rows * columns * n, chunks),
        out_shape=(
            jax.ShapeDtypeStruct(tiles.shape, jnp.float32),
            jax.ShapeDtypeStruct((bands, STATS), jnp.float32),
        ),
        in_specs=[vmem_space] * 2,
        out_specs=[any_space, any_space],
        scratch_shapes=[
            pltpu.VMEM((bands, STATS), jnp.float32),
            pltpu.SemaphoreType.DMA((chunks + 1,)),
        ],
        name="finish",
    )(tiles, stats)
    return out, header.T


def solution(mesh):
    in_specs = (P(None, "dev", None), P(None, "dev", None))
    out_specs = (P("dev", None, None), P())
    return jax.shard_map(
        on_device, mesh=mesh, in_specs=in_specs, out_specs=out_specs, check_vma=False
    )
```

```python
import functools

import jax
import jax.numpy as jnp
from jax import lax
from jax.experimental import pallas as pl
from jax.experimental.pallas import tpu as pltpu
from jax.sharding import PartitionSpec as P

TILE = 512
LANES = 128
SUBLANES = 8
STATS = 5
SLOT = 8
WINDOW = 5
AHEAD = 3

largest_value = 3e38


def schedule(members):
    dims = members.bit_length() - 2
    whole = members // 2 - 1
    near = [1 << dim for dim in range(dims)]
    turns = {}
    for dim in range(dims):
        after = (dim + 1) % dims
        turns.setdefault((1 << dim) + (1 << after), (dim, after))
    relayed = [high for high in turns if high.bit_count() == 2 and high != whole]
    paired = sorted((high for high in range(1, whole) if high > whole - high),
                    key=lambda high: (-max(high.bit_count(), (whole - high).bit_count()), high))
    left = [high for high in range(1, whole) if high.bit_count() > 1 and high not in relayed]
    groups = [[(high, 0) for high in relayed], [(high, 0) for high in near], [(whole, 0)], [(whole, 1)]]
    groups += [[(whole - high, 1), (high, 1)] for high in paired]
    groups += [[(high, 0)] for high in left]
    groups[4].append((0, 1))
    masks, slots = [], []
    for group in groups:
        slots.append(list(range(len(masks), len(masks) + len(group))))
        masks += [high * 2 + core for high, core in group]
    return masks + [0], slots, [turns[high] for high in relayed]


def lane_tables(bands):
    block = LANES // bands
    lane = lax.broadcasted_iota(jnp.int32, (SUBLANES, LANES), 1)
    m, r = lane // bands, lane % bands
    spread = [(r - b + bands) % bands * block + m for b in range(bands)]
    fix = [m * bands + (r + j) % bands for j in range(bands)]
    return r, spread, fix


def permute(x, index):
    return jnp.take_along_axis(x, index, axis=1, mode="promise_in_bounds")


def merge_rows(stats):
    which = lax.broadcasted_iota(jnp.int32, (1, LANES), 1) % SLOT
    low = jnp.min(stats, axis=0, keepdims=True)
    high = jnp.max(stats, axis=0, keepdims=True)
    total = jnp.sum(stats, axis=0, keepdims=True)
    return jnp.where(which == 0, low, jnp.where(which == 1, high, total))


def exchange(n, members, pix_ref, flag_ref, out_ref, stat_out, pix, flag, send, row, rows_in,
             relay, load_sem, send_sem, relay_send, relay_recv, recv_sem, row_send, row_recv, reach, cross):
    bands, rows, _ = pix_ref.shape
    bits = members.bit_length() - 1
    groups = n // members
    me = lax.axis_index("dev")
    position = me % members
    first = me - position
    keeper = 1
    turns = [(1 - 2 * (position // (1 << bit) % 2)) * (1 << bit) for bit in range(bits)]
    masks, slots, bends = schedule(members)
    lead, soon = slots[0], slots[1]

    def peer(mask):
        where = position
        for bit in range(bits):
            if mask >> bit & 1:
                where = where + turns[bit]
        return where

    where = [peer(mask) for mask in masks]
    late = where[slots[-1][0]] < 2
    for step in slots[-1][1:]:
        late = jnp.logical_or(late, where[step] < 2)
    for a, b in zip(slots[-2], slots[-1]):
        where[a], where[b] = jnp.where(late, where[b], where[a]), jnp.where(late, where[a], where[b])

    def mate(k):
        return first + (position + k) % members

    def twin(k):
        return (me + k * members) % n

    def signal(semaphore, whom):
        pl.semaphore_signal(semaphore, inc=1, device_id=(whom,),
                            device_id_type=pl.DeviceIdType.MESH)

    def loads(step, where):
        columns = pl.ds(pl.multiple_of(where * TILE, TILE), TILE)
        return (
            pltpu.make_async_copy(pix_ref.at[:, :, columns], pix.at[step], load_sem.at[0, step]),
            pltpu.make_async_copy(flag_ref.at[:, :, columns], flag.at[step], load_sem.at[1, step]),
        )

    def start_loads(steps):
        for step in steps:
            for copy in loads(step, where[step]):
                copy.start()

    start_loads(lead)

    def each(lo, hi, act):
        def body(k, _):
            act(k)
            return 0

        lax.fori_loop(lo, hi, body, 0)

    barrier = pltpu.get_barrier_semaphore()
    close = [1 << bit for bit in range(bits)]
    for mask in close:
        signal(barrier, first + peer(mask))

    @pl.when(position == keeper)
    def _():
        each(1, groups, lambda k: signal(barrier, twin(k)))


    def widen(level):
        for mask in close:
            signal(reach.at[level], first + peer(mask))

    def copy_to(source, target, send_to, receive, whom):
        return pltpu.make_async_remote_copy(
            src_ref=source,
            dst_ref=target,
            send_sem=send_to,
            recv_sem=receive,
            device_id=(first + whom,),
            device_id_type=pl.DeviceIdType.MESH,
        )

    def landing(sender):
        return out_ref.at[0, pl.ds(pl.multiple_of(sender * rows, rows), rows)]

    def outbound(step, top=0, height=rows):
        return copy_to(
            send.at[step, pl.ds(top, height)], relay.at[step, pl.ds(top, height)],
            send_sem.at[step], relay_recv.at[step], peer(2 << bends[step][0]),
        )

    def forward(step):
        start, after = bends[step]
        return copy_to(
            relay.at[step], landing(peer(2 << start)), relay_send.at[step], recv_sem, peer(2 << after)
        )

    def delivery(step, top=0, height=rows):
        start = pl.multiple_of(position * rows + top, SUBLANES)
        return copy_to(
            send.at[step, pl.ds(top, height)], out_ref.at[0, pl.ds(start, height)],
            send_sem.at[step], recv_sem, where[step],
        )

    half = rows // 2 // SUBLANES * SUBLANES

    residue, spread, fix = lane_tables(bands)

    def wait_loads(step):
        for copy in loads(step, 0):
            copy.wait()

    def work(step, tops, totals, target):
        totals = list(totals)
        for top in tops:
            for left in range(0, TILE, LANES):
                spread_bands = []
                for b in range(bands):
                    x = pix[step, b, top:top + SUBLANES, left:left + LANES]
                    usable = flag[step, b, top:top + SUBLANES, left:left + LANES] == 1
                    filled = jnp.where(usable, x, 0.0)
                    low, high, count, total, squares = totals[b * STATS:(b + 1) * STATS]
                    totals[b * STATS:(b + 1) * STATS] = (
                        jnp.minimum(low, jnp.where(usable, x, largest_value)),
                        jnp.maximum(high, jnp.where(usable, x, -largest_value)),
                        count + jnp.where(usable, 1.0, 0.0),
                        total + filled,
                        squares + filled * filled,
                    )
                    spread_bands.append(permute(filled, spread[b]))
                for j in range(bands):
                    mixed = spread_bands[(bands - j) % bands]
                    for r in range(1, bands):
                        mixed = jnp.where(residue == r, spread_bands[(r - j) % bands], mixed)
                    if j:
                        mixed = permute(mixed, fix[j])
                    target(top, left * bands + j * LANES, mixed)
        return tuple(totals)

    def to_send(step):
        def put(top, left, value):
            send[step, top:top + SUBLANES, left:left + LANES] = value
        return put

    tops = range(0, rows, SUBLANES)

    def work_only(step, totals):
        wait_loads(step)
        return work(step, tops, totals, to_send(step))

    zero = jnp.zeros((SUBLANES, LANES), jnp.float32)
    totals = (zero + largest_value, zero - largest_value, zero, zero, zero) * bands
    for step in lead:
        wait_loads(step)
    for top in tops:
        for step in lead:
            totals = work(step, (top,), totals, to_send(step))
        if top == 0:
            pl.semaphore_wait(barrier, len(close) + jnp.where(position == keeper, groups - 1, 0))
            widen(0)
        for step in lead:
            outbound(step, top, SUBLANES).start()
        if top == 0:
            start_loads(range(len(lead), members))
    done = len(lead)
    for level in range(bits - 1):
        pl.semaphore_wait(reach.at[level], bits)
        if level < bits - 2:
            widen(level + 1)
        if level == 0:
            for step in soon:
                totals = work_only(step, totals)
                delivery(step).start()
                done += 1
        if level == bits - 3:
            for step in slots[2]:
                delivery(step).start()
        if level < bits - 2:
            totals = lax.fori_loop(done, done + AHEAD, work_only, totals)
            done += AHEAD

    @pl.when(position == keeper)
    def _():
        each(1, groups, lambda k: signal(cross, twin(k)))

    totals = lax.fori_loop(done, members - 1, work_only, totals)

    own = pl.multiple_of(position * rows, rows)

    def to_own(top, left, value):
        out_ref[0, pl.ds(own + top, SUBLANES), left:left + LANES] = value

    wait_loads(members - 1)
    totals = work(members - 1, tops, totals, to_own)

    lane = lax.broadcasted_iota(jnp.int32, (1, LANES), 1)
    line = jnp.zeros((1, LANES), jnp.float32)
    for b in range(bands):
        for s, reduce in enumerate((jnp.min, jnp.max, jnp.sum, jnp.sum, jnp.sum)):
            value = totals[b * STATS + s]
            value = reduce(reduce(value, axis=0, keepdims=True), axis=1, keepdims=True)
            line = jnp.where(lane == b * SLOT + s, value, line)
    row[0] = line
    rows_in[members - 1] = line

    group = me // members

    def row_copy(source, target, stage, whom):
        return pltpu.make_async_remote_copy(
            src_ref=source,
            dst_ref=target,
            send_sem=row_send.at[stage],
            recv_sem=row_recv.at[stage],
            device_id=(whom,),
            device_id_type=pl.DeviceIdType.MESH,
        )

    def to_keeper():
        return row_copy(row.at[0], rows_in.at[(position - keeper + members - 1) % members], 0, first + keeper)

    def to_other(k):
        return row_copy(row.at[1], stat_out.at[group], 1, (me + k) % n)

    @pl.when(position != keeper)
    def _():
        to_keeper().start()

    def share():
        others = rows_in.at[pl.ds(0, members - 1)]
        pltpu.make_async_copy(others, others, row_recv.at[0]).wait()
        merged = merge_rows(rows_in[0:members, 0, :])
        row[1] = merged
        stat_out[pl.ds(group, 1)] = merged[None]
        if groups > 1:
            pl.semaphore_wait(cross, groups - 1)
        each(1, n, lambda k: to_other(k).start())

    sends = [
        [outbound(step) for step in lead],
        [delivery(step) for step in soon],
        [delivery(step) for step in slots[2]],
        [forward(step) for step in lead],
        *([delivery(step) for step in slot] for slot in slots[3:]),
    ]
    started = 3
    for k in range(started, len(sends)):
        for copy in sends[k - WINDOW] if k >= WINDOW else ():
            copy.wait_send()
        if k == 3:
            for step in lead:
                outbound(step).wait_recv()
        for copy in sends[k]:
            copy.start()
        if k == 5:
            pl.when(position == keeper)(share)
    for k in range(max(len(sends) - WINDOW, 0), len(sends)):
        for copy in sends[k]:
            copy.wait_send()

    @pl.when(position == keeper)
    def _():
        sent = rows_in.at[pl.ds(0, n - 1)]
        pltpu.make_async_copy(sent, sent, row_send.at[1]).wait()
        if groups > 1:
            others = stat_out.at[pl.ds(0, groups - 1)]
            pltpu.make_async_copy(others, others, row_recv.at[1]).wait()

    @pl.when(position != keeper)
    def _():
        to_keeper().wait_send()
        pltpu.make_async_copy(stat_out, stat_out, row_recv.at[1]).wait()

    arrived = out_ref.at[0, pl.ds(0, (members - 1) * rows)]
    pltpu.make_async_copy(arrived, arrived, recv_sem).wait()


def finish(bands, cell_total, chunks, tiles_ref, stats_ref, out_ref, header_ref, header, sem):
    height = tiles_ref.shape[1] // chunks
    copies = [
        pltpu.make_async_copy(
            tiles_ref.at[:, pl.ds(c * height, height)],
            out_ref.at[:, pl.ds(c * height, height)],
            sem.at[c],
        )
        for c in range(chunks)
    ]
    for copy in copies:
        copy.start()
    stats = stats_ref[:, 0, :]
    low = jnp.min(stats, axis=0, keepdims=True)
    high = jnp.max(stats, axis=0, keepdims=True)
    total = jnp.sum(stats, axis=0, keepdims=True)
    which = lax.broadcasted_iota(jnp.int32, (1, LANES), 1) % SLOT
    count = jnp.where(which == 2, total, 0.0)
    divisor = jnp.maximum(pltpu.roll(count, 1, 1) + pltpu.roll(count, 2, 1), 1.0)
    mean = total / divisor
    average = pltpu.roll(mean, 1, 1)
    deviation = jnp.sqrt(jnp.maximum(mean - average * average, 0.25))
    values = jnp.where(which == 3, mean, deviation)
    values = jnp.where(which == 2, total / cell_total, values)
    values = jnp.where(which == 1, high, values)
    values = jnp.where(which == 0, low, values)
    for b in range(bands):
        header[b:b + 1, :] = values[:, b * SLOT:b * SLOT + STATS]
    header_copy = pltpu.make_async_copy(header, header_ref, sem.at[chunks])
    header_copy.start()
    for copy in copies:
        copy.wait()
    header_copy.wait()


def on_device(pixels, valid_flags):
    bands, rows, columns = pixels.shape
    n = lax.axis_size("dev")
    members = columns // TILE
    relays = len(schedule(members)[2])
    any_space = pl.BlockSpec(memory_space=pl.ANY)
    vmem_space = pl.BlockSpec(memory_space=pltpu.VMEM)
    tiles, stats = pl.pallas_call(
        functools.partial(exchange, n, members),
        out_shape=(
            pltpu.VMEM((1, members * rows, TILE * bands), jnp.float32),
            pltpu.VMEM((n // members, 1, LANES), jnp.float32),
        ),
        in_specs=[any_space] * 2,
        out_specs=[vmem_space] * 2,
        scratch_shapes=[
            pltpu.VMEM((members, bands, rows, TILE), jnp.float32),
            pltpu.VMEM((members, bands, rows, TILE), jnp.int32),
            pltpu.VMEM((members - 1, rows, TILE * bands), jnp.float32),
            pltpu.VMEM((2, 1, LANES), jnp.float32),
            pltpu.VMEM((n, 1, LANES), jnp.float32),
            pltpu.VMEM((relays, rows, TILE * bands), jnp.float32),
            pltpu.SemaphoreType.DMA((2, members)),
            pltpu.SemaphoreType.DMA((members - 1,)),
            pltpu.SemaphoreType.DMA((relays,)),
            pltpu.SemaphoreType.DMA((relays,)),
            pltpu.SemaphoreType.DMA,
            pltpu.SemaphoreType.DMA((2,)),
            pltpu.SemaphoreType.DMA((2,)),
            pltpu.SemaphoreType.REGULAR((members.bit_length() - 2,)),
            pltpu.SemaphoreType.REGULAR,
        ],
        compiler_params=pltpu.CompilerParams(collective_id=0, has_side_effects=True),
        name="exchange",
    )(pixels, valid_flags)
    chunks = 4
    tiles = pltpu.with_memory_space_constraint(tiles, pltpu.VMEM)
    stats = pltpu.with_memory_space_constraint(stats, pltpu.VMEM)
    out, header = pl.pallas_call(
        functools.partial(finish, bands, rows * columns * n, chunks),
        out_shape=(
            jax.ShapeDtypeStruct(tiles.shape, jnp.float32),
            jax.ShapeDtypeStruct((bands, STATS), jnp.float32),
        ),
        in_specs=[vmem_space] * 2,
        out_specs=[any_space, any_space],
        scratch_shapes=[
            pltpu.VMEM((bands, STATS), jnp.float32),
            pltpu.SemaphoreType.DMA((chunks + 1,)),
        ],
        name="finish",
    )(tiles, stats)
    return out, header.T


def solution(mesh):
    in_specs = (P(None, "dev", None), P(None, "dev", None))
    out_specs = (P("dev", None, None), P())
    return jax.shard_map(
        on_device, mesh=mesh, in_specs=in_specs, out_specs=out_specs, check_vma=False
    )
```

```python
import functools

import jax
import jax.numpy as jnp
from jax import lax
from jax.experimental import pallas as pl
from jax.experimental.pallas import tpu as pltpu
from jax.sharding import PartitionSpec as P

TILE = 512
LANES = 128
SUBLANES = 8
STATS = 5
SLOT = 8
WINDOW = 5
AHEAD = 3

largest_value = 3e38


def schedule(members):
    dims = members.bit_length() - 2
    whole = members // 2 - 1
    near = [1 << dim for dim in range(dims)]
    turns = {}
    for dim in range(dims):
        after = (dim + 1) % dims
        turns.setdefault((1 << dim) + (1 << after), (dim, after))
    relayed = [high for high in turns if high.bit_count() == 2 and high != whole]
    paired = sorted((high for high in range(1, whole) if high > whole - high),
                    key=lambda high: (-max(high.bit_count(), (whole - high).bit_count()), high))
    left = [high for high in range(1, whole) if high.bit_count() > 1 and high not in relayed]
    groups = [[(high, 0) for high in relayed], [(high, 0) for high in near], [(whole, 0)], [(whole, 1)]]
    groups += [[(whole - high, 1), (high, 1)] for high in paired]
    groups += [[(high, 0)] for high in left]
    groups[4].append((0, 1))
    masks, slots = [], []
    for group in groups:
        slots.append(list(range(len(masks), len(masks) + len(group))))
        masks += [high * 2 + core for high, core in group]
    return masks + [0], slots, [turns[high] for high in relayed]


def lane_tables(bands):
    block = LANES // bands
    lane = lax.broadcasted_iota(jnp.int32, (SUBLANES, LANES), 1)
    m, r = lane // bands, lane % bands
    spread = [(r - b + bands) % bands * block + m for b in range(bands)]
    fix = [m * bands + (r + j) % bands for j in range(bands)]
    return r, spread, fix


def permute(x, index):
    return jnp.take_along_axis(x, index, axis=1, mode="promise_in_bounds")


def merge_rows(stats):
    which = lax.broadcasted_iota(jnp.int32, (1, LANES), 1) % SLOT
    low = jnp.min(stats, axis=0, keepdims=True)
    high = jnp.max(stats, axis=0, keepdims=True)
    total = jnp.sum(stats, axis=0, keepdims=True)
    return jnp.where(which == 0, low, jnp.where(which == 1, high, total))


def exchange(n, members, pix_ref, flag_ref, out_ref, stat_out, pix, flag, send, row, rows_in,
             relay, load_sem, send_sem, relay_send, relay_recv, recv_sem, row_send, row_recv, reach, cross):
    bands, rows, _ = pix_ref.shape
    bits = members.bit_length() - 1
    groups = n // members
    me = lax.axis_index("dev")
    position = me % members
    first = me - position
    keeper = 1
    turns = [(1 - 2 * (position // (1 << bit) % 2)) * (1 << bit) for bit in range(bits)]
    masks, slots, bends = schedule(members)
    lead, soon = slots[0], slots[1]

    def peer(mask):
        where = position
        for bit in range(bits):
            if mask >> bit & 1:
                where = where + turns[bit]
        return where

    where = [peer(mask) for mask in masks]
    late = where[slots[-1][0]] < 2
    for step in slots[-1][1:]:
        late = jnp.logical_or(late, where[step] < 2)
    for a, b in zip(slots[-2], slots[-1]):
        where[a], where[b] = jnp.where(late, where[b], where[a]), jnp.where(late, where[a], where[b])

    last = position == members - 2
    a, b = slots[-1][1], slots[-3][1]
    where[a], where[b] = jnp.where(last, where[b], where[a]), jnp.where(last, where[a], where[b])

    def mate(k):
        return first + (position + k) % members

    def twin(k):
        return (me + k * members) % n

    def signal(semaphore, whom):
        pl.semaphore_signal(semaphore, inc=1, device_id=(whom,),
                            device_id_type=pl.DeviceIdType.MESH)

    def loads(step, where):
        columns = pl.ds(pl.multiple_of(where * TILE, TILE), TILE)
        return (
            pltpu.make_async_copy(pix_ref.at[:, :, columns], pix.at[step], load_sem.at[0, step]),
            pltpu.make_async_copy(flag_ref.at[:, :, columns], flag.at[step], load_sem.at[1, step]),
        )

    def start_loads(steps):
        for step in steps:
            for copy in loads(step, where[step]):
                copy.start()

    start_loads(lead)

    def each(lo, hi, act):
        def body(k, _):
            act(k)
            return 0

        lax.fori_loop(lo, hi, body, 0)

    barrier = pltpu.get_barrier_semaphore()
    close = [1 << bit for bit in range(bits)]
    for mask in close:
        signal(barrier, first + peer(mask))

    @pl.when(position == keeper)
    def _():
        each(1, groups, lambda k: signal(barrier, twin(k)))


    def widen(level):
        for mask in close:
            signal(reach.at[level], first + peer(mask))

    def copy_to(source, target, send_to, receive, whom):
        return pltpu.make_async_remote_copy(
            src_ref=source,
            dst_ref=target,
            send_sem=send_to,
            recv_sem=receive,
            device_id=(first + whom,),
            device_id_type=pl.DeviceIdType.MESH,
        )

    def landing(sender):
        return out_ref.at[0, pl.ds(pl.multiple_of(sender * rows, rows), rows)]

    def outbound(step, top=0, height=rows):
        return copy_to(
            send.at[step, pl.ds(top, height)], relay.at[step, pl.ds(top, height)],
            send_sem.at[step], relay_recv.at[step], peer(2 << bends[step][0]),
        )

    def forward(step):
        start, after = bends[step]
        return copy_to(
            relay.at[step], landing(peer(2 << start)), relay_send.at[step], recv_sem, peer(2 << after)
        )

    def delivery(step, top=0, height=rows):
        start = pl.multiple_of(position * rows + top, SUBLANES)
        return copy_to(
            send.at[step, pl.ds(top, height)], out_ref.at[0, pl.ds(start, height)],
            send_sem.at[step], recv_sem, where[step],
        )

    half = rows // 2 // SUBLANES * SUBLANES

    residue, spread, fix = lane_tables(bands)

    def wait_loads(step):
        for copy in loads(step, 0):
            copy.wait()

    def work(step, tops, totals, target):
        totals = list(totals)
        for top in tops:
            for left in range(0, TILE, LANES):
                spread_bands = []
                for b in range(bands):
                    x = pix[step, b, top:top + SUBLANES, left:left + LANES]
                    usable = flag[step, b, top:top + SUBLANES, left:left + LANES] == 1
                    filled = jnp.where(usable, x, 0.0)
                    low, high, count, total, squares = totals[b * STATS:(b + 1) * STATS]
                    totals[b * STATS:(b + 1) * STATS] = (
                        jnp.minimum(low, jnp.where(usable, x, largest_value)),
                        jnp.maximum(high, jnp.where(usable, x, -largest_value)),
                        count + jnp.where(usable, 1.0, 0.0),
                        total + filled,
                        squares + filled * filled,
                    )
                    spread_bands.append(permute(filled, spread[b]))
                for j in range(bands):
                    mixed = spread_bands[(bands - j) % bands]
                    for r in range(1, bands):
                        mixed = jnp.where(residue == r, spread_bands[(r - j) % bands], mixed)
                    if j:
                        mixed = permute(mixed, fix[j])
                    target(top, left * bands + j * LANES, mixed)
        return tuple(totals)

    def to_send(step):
        def put(top, left, value):
            send[step, top:top + SUBLANES, left:left + LANES] = value
        return put

    tops = range(0, rows, SUBLANES)

    def work_only(step, totals):
        wait_loads(step)
        return work(step, tops, totals, to_send(step))

    zero = jnp.zeros((SUBLANES, LANES), jnp.float32)
    totals = (zero + largest_value, zero - largest_value, zero, zero, zero) * bands
    for step in lead:
        wait_loads(step)
    for top in tops:
        for step in lead:
            totals = work(step, (top,), totals, to_send(step))
        if top == 0:
            pl.semaphore_wait(barrier, len(close) + jnp.where(position == keeper, groups - 1, 0))
            widen(0)
        for step in lead:
            outbound(step, top, SUBLANES).start()
        if top == 0:
            start_loads(range(len(lead), members))
    done = len(lead)
    for level in range(bits - 1):
        pl.semaphore_wait(reach.at[level], bits)
        if level < bits - 2:
            widen(level + 1)
        if level == 0:
            for step in soon:
                totals = work_only(step, totals)
                delivery(step).start()
                done += 1
        if level == bits - 3:
            for step in slots[2]:
                delivery(step).start()
        if level < bits - 2:
            totals = lax.fori_loop(done, done + AHEAD, work_only, totals)
            done += AHEAD

    @pl.when(position == keeper)
    def _():
        each(1, groups, lambda k: signal(cross, twin(k)))

    totals = lax.fori_loop(done, members - 1, work_only, totals)

    own = pl.multiple_of(position * rows, rows)

    def to_own(top, left, value):
        out_ref[0, pl.ds(own + top, SUBLANES), left:left + LANES] = value

    wait_loads(members - 1)
    totals = work(members - 1, tops, totals, to_own)

    lane = lax.broadcasted_iota(jnp.int32, (1, LANES), 1)
    line = jnp.zeros((1, LANES), jnp.float32)
    for b in range(bands):
        for s, reduce in enumerate((jnp.min, jnp.max, jnp.sum, jnp.sum, jnp.sum)):
            value = totals[b * STATS + s]
            value = reduce(reduce(value, axis=0, keepdims=True), axis=1, keepdims=True)
            line = jnp.where(lane == b * SLOT + s, value, line)
    row[0] = line
    rows_in[members - 1] = line

    group = me // members

    def row_copy(source, target, stage, whom):
        return pltpu.make_async_remote_copy(
            src_ref=source,
            dst_ref=target,
            send_sem=row_send.at[stage],
            recv_sem=row_recv.at[stage],
            device_id=(whom,),
            device_id_type=pl.DeviceIdType.MESH,
        )

    def to_keeper():
        return row_copy(row.at[0], rows_in.at[(position - keeper + members - 1) % members], 0, first + keeper)

    def to_other(k):
        return row_copy(row.at[1], stat_out.at[group], 1, (me + k) % n)

    @pl.when(position != keeper)
    def _():
        to_keeper().start()

    def share():
        others = rows_in.at[pl.ds(0, members - 1)]
        pltpu.make_async_copy(others, others, row_recv.at[0]).wait()
        merged = merge_rows(rows_in[0:members, 0, :])
        row[1] = merged
        stat_out[pl.ds(group, 1)] = merged[None]
        if groups > 1:
            pl.semaphore_wait(cross, groups - 1)
        each(1, n, lambda k: to_other(k).start())

    sends = [
        [outbound(step) for step in lead],
        [delivery(step) for step in soon],
        [delivery(step) for step in slots[2]],
        [forward(step) for step in lead],
        *([delivery(step) for step in slot] for slot in slots[3:]),
    ]
    started = 3
    for k in range(started, len(sends)):
        for copy in sends[k - WINDOW] if k >= WINDOW else ():
            copy.wait_send()
        if k == 3:
            for step in lead:
                outbound(step).wait_recv()
        for copy in sends[k]:
            copy.start()
        if k == 5:
            pl.when(position == keeper)(share)
    for k in range(max(len(sends) - WINDOW, 0), len(sends)):
        for copy in sends[k]:
            copy.wait_send()

    @pl.when(position == keeper)
    def _():
        sent = rows_in.at[pl.ds(0, n - 1)]
        pltpu.make_async_copy(sent, sent, row_send.at[1]).wait()
        if groups > 1:
            others = stat_out.at[pl.ds(0, groups - 1)]
            pltpu.make_async_copy(others, others, row_recv.at[1]).wait()

    @pl.when(position != keeper)
    def _():
        to_keeper().wait_send()
        pltpu.make_async_copy(stat_out, stat_out, row_recv.at[1]).wait()

    arrived = out_ref.at[0, pl.ds(0, (members - 1) * rows)]
    pltpu.make_async_copy(arrived, arrived, recv_sem).wait()


def finish(bands, cell_total, chunks, tiles_ref, stats_ref, out_ref, header_ref, header, sem):
    height = tiles_ref.shape[1] // chunks
    copies = [
        pltpu.make_async_copy(
            tiles_ref.at[:, pl.ds(c * height, height)],
            out_ref.at[:, pl.ds(c * height, height)],
            sem.at[c],
        )
        for c in range(chunks)
    ]
    for copy in copies:
        copy.start()
    stats = stats_ref[:, 0, :]
    low = jnp.min(stats, axis=0, keepdims=True)
    high = jnp.max(stats, axis=0, keepdims=True)
    total = jnp.sum(stats, axis=0, keepdims=True)
    which = lax.broadcasted_iota(jnp.int32, (1, LANES), 1) % SLOT
    count = jnp.where(which == 2, total, 0.0)
    divisor = jnp.maximum(pltpu.roll(count, 1, 1) + pltpu.roll(count, 2, 1), 1.0)
    mean = total / divisor
    average = pltpu.roll(mean, 1, 1)
    deviation = jnp.sqrt(jnp.maximum(mean - average * average, 0.25))
    values = jnp.where(which == 3, mean, deviation)
    values = jnp.where(which == 2, total / cell_total, values)
    values = jnp.where(which == 1, high, values)
    values = jnp.where(which == 0, low, values)
    for b in range(bands):
        header[b:b + 1, :] = values[:, b * SLOT:b * SLOT + STATS]
    header_copy = pltpu.make_async_copy(header, header_ref, sem.at[chunks])
    header_copy.start()
    for copy in copies:
        copy.wait()
    header_copy.wait()


def on_device(pixels, valid_flags):
    bands, rows, columns = pixels.shape
    n = lax.axis_size("dev")
    members = columns // TILE
    relays = len(schedule(members)[2])
    any_space = pl.BlockSpec(memory_space=pl.ANY)
    vmem_space = pl.BlockSpec(memory_space=pltpu.VMEM)
    tiles, stats = pl.pallas_call(
        functools.partial(exchange, n, members),
        out_shape=(
            pltpu.VMEM((1, members * rows, TILE * bands), jnp.float32),
            pltpu.VMEM((n // members, 1, LANES), jnp.float32),
        ),
        in_specs=[any_space] * 2,
        out_specs=[vmem_space] * 2,
        scratch_shapes=[
            pltpu.VMEM((members, bands, rows, TILE), jnp.float32),
            pltpu.VMEM((members, bands, rows, TILE), jnp.int32),
            pltpu.VMEM((members - 1, rows, TILE * bands), jnp.float32),
            pltpu.VMEM((2, 1, LANES), jnp.float32),
            pltpu.VMEM((n, 1, LANES), jnp.float32),
            pltpu.VMEM((relays, rows, TILE * bands), jnp.float32),
            pltpu.SemaphoreType.DMA((2, members)),
            pltpu.SemaphoreType.DMA((members - 1,)),
            pltpu.SemaphoreType.DMA((relays,)),
            pltpu.SemaphoreType.DMA((relays,)),
            pltpu.SemaphoreType.DMA,
            pltpu.SemaphoreType.DMA((2,)),
            pltpu.SemaphoreType.DMA((2,)),
            pltpu.SemaphoreType.REGULAR((members.bit_length() - 2,)),
            pltpu.SemaphoreType.REGULAR,
        ],
        compiler_params=pltpu.CompilerParams(collective_id=0, has_side_effects=True),
        name="exchange",
    )(pixels, valid_flags)
    chunks = 2
    tiles = pltpu.with_memory_space_constraint(tiles, pltpu.VMEM)
    stats = pltpu.with_memory_space_constraint(stats, pltpu.VMEM)
    out, header = pl.pallas_call(
        functools.partial(finish, bands, rows * columns * n, chunks),
        out_shape=(
            jax.ShapeDtypeStruct(tiles.shape, jnp.float32),
            jax.ShapeDtypeStruct((bands, STATS), jnp.float32),
        ),
        in_specs=[vmem_space] * 2,
        out_specs=[any_space, any_space],
        scratch_shapes=[
            pltpu.VMEM((bands, STATS), jnp.float32),
            pltpu.SemaphoreType.DMA((chunks + 1,)),
        ],
        name="finish",
    )(tiles, stats)
    return out, header.T


def solution(mesh):
    in_specs = (P(None, "dev", None), P(None, "dev", None))
    out_specs = (P("dev", None, None), P())
    return jax.shard_map(
        on_device, mesh=mesh, in_specs=in_specs, out_specs=out_specs, check_vma=False
    )
```

```python
import functools

import jax
import jax.numpy as jnp
from jax import lax
from jax.experimental import pallas as pl
from jax.experimental.pallas import tpu as pltpu
from jax.sharding import PartitionSpec as P

TILE = 512
LANES = 128
SUBLANES = 8
STATS = 5
SLOT = 8
WINDOW = 5
AHEAD = 3

largest_value = 3e38


def schedule(members):
    dims = members.bit_length() - 2
    whole = members // 2 - 1
    near = [1 << dim for dim in range(dims)]
    turns = {}
    for dim in range(dims):
        after = (dim + 1) % dims
        turns.setdefault((1 << dim) + (1 << after), (dim, after))
    relayed = [high for high in turns if high.bit_count() == 2 and high != whole]
    paired = sorted((high for high in range(1, whole) if high > whole - high),
                    key=lambda high: (-max(high.bit_count(), (whole - high).bit_count()), high))
    left = [high for high in range(1, whole) if high.bit_count() > 1 and high not in relayed]
    groups = [[(high, 0) for high in relayed], [(high, 0) for high in near], [(whole, 0)], [(whole, 1)]]
    groups += [[(whole - high, 1), (high, 1)] for high in paired]
    groups += [[(high, 0)] for high in left]
    groups[4].append((0, 1))
    masks, slots = [], []
    for group in groups:
        slots.append(list(range(len(masks), len(masks) + len(group))))
        masks += [high * 2 + core for high, core in group]
    return masks + [0], slots, [turns[high] for high in relayed]


def lane_tables(bands):
    block = LANES // bands
    lane = lax.broadcasted_iota(jnp.int32, (SUBLANES, LANES), 1)
    m, r = lane // bands, lane % bands
    spread = [(r - b + bands) % bands * block + m for b in range(bands)]
    fix = [m * bands + (r + j) % bands for j in range(bands)]
    return r, spread, fix


def permute(x, index):
    return jnp.take_along_axis(x, index, axis=1, mode="promise_in_bounds")


def merge_rows(stats):
    which = lax.broadcasted_iota(jnp.int32, (1, LANES), 1) % SLOT
    low = jnp.min(stats, axis=0, keepdims=True)
    high = jnp.max(stats, axis=0, keepdims=True)
    total = jnp.sum(stats, axis=0, keepdims=True)
    return jnp.where(which == 0, low, jnp.where(which == 1, high, total))


def exchange(n, members, pix_ref, flag_ref, out_ref, stat_out, pix, flag, send, row, rows_in,
             relay, load_sem, send_sem, relay_send, relay_recv, recv_sem, row_send, row_recv, reach, cross):
    bands, rows, _ = pix_ref.shape
    bits = members.bit_length() - 1
    groups = n // members
    me = lax.axis_index("dev")
    position = me % members
    first = me - position
    keeper = 1
    turns = [(1 - 2 * (position // (1 << bit) % 2)) * (1 << bit) for bit in range(bits)]
    masks, slots, bends = schedule(members)
    lead, soon = slots[0], slots[1]

    def peer(mask):
        where = position
        for bit in range(bits):
            if mask >> bit & 1:
                where = where + turns[bit]
        return where

    where = [peer(mask) for mask in masks]
    late = where[slots[-1][0]] < 2
    for step in slots[-1][1:]:
        late = jnp.logical_or(late, where[step] < 2)
    for a, b in zip(slots[-2], slots[-1]):
        where[a], where[b] = jnp.where(late, where[b], where[a]), jnp.where(late, where[a], where[b])

    last = position == members - 2
    a, b = slots[-1][1], slots[-3][1]
    where[a], where[b] = jnp.where(last, where[b], where[a]), jnp.where(last, where[a], where[b])

    def mate(k):
        return first + (position + k) % members

    def twin(k):
        return (me + k * members) % n

    def signal(semaphore, whom):
        pl.semaphore_signal(semaphore, inc=1, device_id=(whom,),
                            device_id_type=pl.DeviceIdType.MESH)

    def loads(step, where):
        columns = pl.ds(pl.multiple_of(where * TILE, TILE), TILE)
        return (
            pltpu.make_async_copy(pix_ref.at[:, :, columns], pix.at[step], load_sem.at[0, step]),
            pltpu.make_async_copy(flag_ref.at[:, :, columns], flag.at[step], load_sem.at[1, step]),
        )

    def start_loads(steps):
        for step in steps:
            for copy in loads(step, where[step]):
                copy.start()

    start_loads(lead)

    def each(lo, hi, act):
        def body(k, _):
            act(k)
            return 0

        lax.fori_loop(lo, hi, body, 0)

    barrier = pltpu.get_barrier_semaphore()
    close = [1 << bit for bit in range(bits)]
    for mask in close:
        signal(barrier, first + peer(mask))

    @pl.when(position == keeper)
    def _():
        each(1, groups, lambda k: signal(barrier, twin(k)))


    def widen(level):
        for mask in close:
            signal(reach.at[level], first + peer(mask))

    def copy_to(source, target, send_to, receive, whom):
        return pltpu.make_async_remote_copy(
            src_ref=source,
            dst_ref=target,
            send_sem=send_to,
            recv_sem=receive,
            device_id=(first + whom,),
            device_id_type=pl.DeviceIdType.MESH,
        )

    def landing(sender):
        return out_ref.at[0, pl.ds(pl.multiple_of(sender * rows, rows), rows)]

    def outbound(step, top=0, height=rows):
        return copy_to(
            send.at[step, pl.ds(top, height)], relay.at[step, pl.ds(top, height)],
            send_sem.at[step], relay_recv.at[step], peer(2 << bends[step][0]),
        )

    def forward(step):
        start, after = bends[step]
        return copy_to(
            relay.at[step], landing(peer(2 << start)), relay_send.at[step], recv_sem, peer(2 << after)
        )

    def delivery(step, top=0, height=rows):
        start = pl.multiple_of(position * rows + top, SUBLANES)
        return copy_to(
            send.at[step, pl.ds(top, height)], out_ref.at[0, pl.ds(start, height)],
            send_sem.at[step], recv_sem, where[step],
        )

    half = rows // 2 // SUBLANES * SUBLANES

    residue, spread, fix = lane_tables(bands)

    def wait_loads(step):
        for copy in loads(step, 0):
            copy.wait()

    def work(step, tops, totals, target):
        totals = list(totals)
        for top in tops:
            for left in range(0, TILE, LANES):
                spread_bands = []
                for b in range(bands):
                    x = pix[step, b, top:top + SUBLANES, left:left + LANES]
                    usable = flag[step, b, top:top + SUBLANES, left:left + LANES] == 1
                    filled = jnp.where(usable, x, 0.0)
                    low, high, count, total, squares = totals[b * STATS:(b + 1) * STATS]
                    totals[b * STATS:(b + 1) * STATS] = (
                        jnp.minimum(low, jnp.where(usable, x, largest_value)),
                        jnp.maximum(high, jnp.where(usable, x, -largest_value)),
                        count + jnp.where(usable, 1.0, 0.0),
                        total + filled,
                        squares + filled * filled,
                    )
                    spread_bands.append(permute(filled, spread[b]))
                for j in range(bands):
                    mixed = spread_bands[(bands - j) % bands]
                    for r in range(1, bands):
                        mixed = jnp.where(residue == r, spread_bands[(r - j) % bands], mixed)
                    if j:
                        mixed = permute(mixed, fix[j])
                    target(top, left * bands + j * LANES, mixed)
        return tuple(totals)

    def to_send(step):
        def put(top, left, value):
            send[step, top:top + SUBLANES, left:left + LANES] = value
        return put

    tops = range(0, rows, SUBLANES)

    def work_only(step, totals):
        wait_loads(step)
        return work(step, tops, totals, to_send(step))

    zero = jnp.zeros((SUBLANES, LANES), jnp.float32)
    totals = (zero + largest_value, zero - largest_value, zero, zero, zero) * bands
    for step in lead:
        wait_loads(step)
    for top in tops:
        for step in lead:
            totals = work(step, (top,), totals, to_send(step))
        if top == 0:
            pl.semaphore_wait(barrier, len(close) + jnp.where(position == keeper, groups - 1, 0))
            widen(0)
        for step in lead:
            outbound(step, top, SUBLANES).start()
        if top == 0:
            start_loads(range(len(lead), members))
    done = len(lead)
    for step in soon:
        totals = work_only(step, totals)
        delivery(step).start()
        done += 1
    for level in range(bits - 1):
        pl.semaphore_wait(reach.at[level], bits)
        if level < bits - 2:
            widen(level + 1)
        if level == bits - 3:
            for step in slots[2]:
                delivery(step).start()
        if level < bits - 2:
            totals = lax.fori_loop(done, done + AHEAD, work_only, totals)
            done += AHEAD

    @pl.when(position == keeper)
    def _():
        each(1, groups, lambda k: signal(cross, twin(k)))

    totals = lax.fori_loop(done, members - 1, work_only, totals)

    own = pl.multiple_of(position * rows, rows)

    def to_own(top, left, value):
        out_ref[0, pl.ds(own + top, SUBLANES), left:left + LANES] = value

    wait_loads(members - 1)
    totals = work(members - 1, tops, totals, to_own)

    lane = lax.broadcasted_iota(jnp.int32, (1, LANES), 1)
    line = jnp.zeros((1, LANES), jnp.float32)
    for b in range(bands):
        for s, reduce in enumerate((jnp.min, jnp.max, jnp.sum, jnp.sum, jnp.sum)):
            value = totals[b * STATS + s]
            value = reduce(reduce(value, axis=0, keepdims=True), axis=1, keepdims=True)
            line = jnp.where(lane == b * SLOT + s, value, line)
    row[0] = line
    rows_in[members - 1] = line

    group = me // members

    def row_copy(source, target, stage, whom):
        return pltpu.make_async_remote_copy(
            src_ref=source,
            dst_ref=target,
            send_sem=row_send.at[stage],
            recv_sem=row_recv.at[stage],
            device_id=(whom,),
            device_id_type=pl.DeviceIdType.MESH,
        )

    def to_keeper():
        return row_copy(row.at[0], rows_in.at[(position - keeper + members - 1) % members], 0, first + keeper)

    def to_other(k):
        return row_copy(row.at[1], stat_out.at[group], 1, (me + k) % n)

    @pl.when(position != keeper)
    def _():
        to_keeper().start()

    def share():
        others = rows_in.at[pl.ds(0, members - 1)]
        pltpu.make_async_copy(others, others, row_recv.at[0]).wait()
        merged = merge_rows(rows_in[0:members, 0, :])
        row[1] = merged
        stat_out[pl.ds(group, 1)] = merged[None]
        if groups > 1:
            pl.semaphore_wait(cross, groups - 1)
        each(1, n, lambda k: to_other(k).start())

    sends = [
        [outbound(step) for step in lead],
        [delivery(step) for step in soon],
        [delivery(step) for step in slots[2]],
        [forward(step) for step in lead],
        *([delivery(step) for step in slot] for slot in slots[3:]),
    ]
    started = 3
    for k in range(started, len(sends)):
        for copy in sends[k - WINDOW] if k >= WINDOW else ():
            copy.wait_send()
        if k == 3:
            for step in lead:
                outbound(step).wait_recv()
        for copy in sends[k]:
            copy.start()
        if k == 5:
            pl.when(position == keeper)(share)
    for k in range(max(len(sends) - WINDOW, 0), len(sends)):
        for copy in sends[k]:
            copy.wait_send()

    @pl.when(position == keeper)
    def _():
        sent = rows_in.at[pl.ds(0, n - 1)]
        pltpu.make_async_copy(sent, sent, row_send.at[1]).wait()
        if groups > 1:
            others = stat_out.at[pl.ds(0, groups - 1)]
            pltpu.make_async_copy(others, others, row_recv.at[1]).wait()

    @pl.when(position != keeper)
    def _():
        to_keeper().wait_send()
        pltpu.make_async_copy(stat_out, stat_out, row_recv.at[1]).wait()

    arrived = out_ref.at[0, pl.ds(0, (members - 1) * rows)]
    pltpu.make_async_copy(arrived, arrived, recv_sem).wait()


def finish(bands, cell_total, chunks, tiles_ref, stats_ref, out_ref, header_ref, header, sem):
    height = tiles_ref.shape[1] // chunks
    copies = [
        pltpu.make_async_copy(
            tiles_ref.at[:, pl.ds(c * height, height)],
            out_ref.at[:, pl.ds(c * height, height)],
            sem.at[c],
        )
        for c in range(chunks)
    ]
    for copy in copies:
        copy.start()
    stats = stats_ref[:, 0, :]
    low = jnp.min(stats, axis=0, keepdims=True)
    high = jnp.max(stats, axis=0, keepdims=True)
    total = jnp.sum(stats, axis=0, keepdims=True)
    which = lax.broadcasted_iota(jnp.int32, (1, LANES), 1) % SLOT
    count = jnp.where(which == 2, total, 0.0)
    divisor = jnp.maximum(pltpu.roll(count, 1, 1) + pltpu.roll(count, 2, 1), 1.0)
    mean = total / divisor
    average = pltpu.roll(mean, 1, 1)
    deviation = jnp.sqrt(jnp.maximum(mean - average * average, 0.25))
    values = jnp.where(which == 3, mean, deviation)
    values = jnp.where(which == 2, total / cell_total, values)
    values = jnp.where(which == 1, high, values)
    values = jnp.where(which == 0, low, values)
    for b in range(bands):
        header[b:b + 1, :] = values[:, b * SLOT:b * SLOT + STATS]
    header_copy = pltpu.make_async_copy(header, header_ref, sem.at[chunks])
    header_copy.start()
    for copy in copies:
        copy.wait()
    header_copy.wait()


def on_device(pixels, valid_flags):
    bands, rows, columns = pixels.shape
    n = lax.axis_size("dev")
    members = columns // TILE
    relays = len(schedule(members)[2])
    any_space = pl.BlockSpec(memory_space=pl.ANY)
    vmem_space = pl.BlockSpec(memory_space=pltpu.VMEM)
    tiles, stats = pl.pallas_call(
        functools.partial(exchange, n, members),
        out_shape=(
            pltpu.VMEM((1, members * rows, TILE * bands), jnp.float32),
            pltpu.VMEM((n // members, 1, LANES), jnp.float32),
        ),
        in_specs=[any_space] * 2,
        out_specs=[vmem_space] * 2,
        scratch_shapes=[
            pltpu.VMEM((members, bands, rows, TILE), jnp.float32),
            pltpu.VMEM((members, bands, rows, TILE), jnp.int32),
            pltpu.VMEM((members - 1, rows, TILE * bands), jnp.float32),
            pltpu.VMEM((2, 1, LANES), jnp.float32),
            pltpu.VMEM((n, 1, LANES), jnp.float32),
            pltpu.VMEM((relays, rows, TILE * bands), jnp.float32),
            pltpu.SemaphoreType.DMA((2, members)),
            pltpu.SemaphoreType.DMA((members - 1,)),
            pltpu.SemaphoreType.DMA((relays,)),
            pltpu.SemaphoreType.DMA((relays,)),
            pltpu.SemaphoreType.DMA,
            pltpu.SemaphoreType.DMA((2,)),
            pltpu.SemaphoreType.DMA((2,)),
            pltpu.SemaphoreType.REGULAR((members.bit_length() - 2,)),
            pltpu.SemaphoreType.REGULAR,
        ],
        compiler_params=pltpu.CompilerParams(collective_id=0, has_side_effects=True),
        name="exchange",
    )(pixels, valid_flags)
    chunks = 2
    tiles = pltpu.with_memory_space_constraint(tiles, pltpu.VMEM)
    stats = pltpu.with_memory_space_constraint(stats, pltpu.VMEM)
    out, header = pl.pallas_call(
        functools.partial(finish, bands, rows * columns * n, chunks),
        out_shape=(
            jax.ShapeDtypeStruct(tiles.shape, jnp.float32),
            jax.ShapeDtypeStruct((bands, STATS), jnp.float32),
        ),
        in_specs=[vmem_space] * 2,
        out_specs=[any_space, any_space],
        scratch_shapes=[
            pltpu.VMEM((bands, STATS), jnp.float32),
            pltpu.SemaphoreType.DMA((chunks + 1,)),
        ],
        name="finish",
    )(tiles, stats)
    return out, header.T


def solution(mesh):
    in_specs = (P(None, "dev", None), P(None, "dev", None))
    out_specs = (P("dev", None, None), P())
    return jax.shard_map(
        on_device, mesh=mesh, in_specs=in_specs, out_specs=out_specs, check_vma=False
    )
```
